8 devices in a mesh: part: 1 (over z), row: 2 (over y), col: 4 (over x, core).
Axes of the slice: x: 2, y: 2, z: 1, core: 2. Of those that a mesh axis runs over, the one named last changes fastest.
Arguments:
- counts: bfloat16 [2048, 65536], P(('part', 'row'), 'col')
- w_init: float32 [2048, 256], P(('part', 'row'))
- h_init: float32 [256, 65536], P('part', 'col')
Outputs:
- output 1: float32 [2048, 256], P(('part', 'row'))
- output 2: float32 [256, 65536], P('part', 'col')
All inputs are finite; a program needn't handle non-finite values.
Results may differ from the reference program's by a relative error of at most 0.001.
Values are sent between devices in bfloat16 or wider.
A program may use at most 1 GiB of HBM per device.

```python
import jax
import jax.numpy as jnp
from jax import lax

DOCS = 2048
VOCAB = 65536
TOPICS = 256
SWEEPS = 6
BLOCK_ROWS = 128


def setup_inputs(seed: int = 0, part: int = 0) -> dict:
    root_key = jax.random.fold_in(jax.random.key(seed), part)
    key_row, key_col, key_cnt, key_w, key_h = jax.random.split(root_key, 5)
    row_level = jax.random.randint(key_row, (DOCS, 1), 1, 5)
    col_level = jax.random.randint(key_col, (1, VOCAB), 1, 5)
    raw_bits = jax.random.randint(key_cnt, (DOCS, VOCAB), 0, 2 ** 20)
    counts = raw_bits % (1 + row_level * col_level)
    init_scale = (3.0 / TOPICS) ** 0.5
    w_init = jax.random.uniform(key_w, (DOCS, TOPICS), jnp.float32, 0.25, 1.75) * init_scale
    h_init = jax.random.uniform(key_h, (TOPICS, VOCAB), jnp.float32, 0.25, 1.75) * init_scale
    return {"counts": counts.astype(jnp.float32).astype(jnp.bfloat16), "w_init": w_init, "h_init": h_init}


def reference(counts, w_init, h_init):
    num_blocks = DOCS // BLOCK_ROWS
    count_blocks = counts.reshape(num_blocks, BLOCK_ROWS, VOCAB)

    def one_sweep(carry_state, sweep_idx):
        w_state, h_state = carry_state
        w_bf = w_state.astype(jnp.bfloat16)
        h_bf = h_state.astype(jnp.bfloat16)
        h_rowsum = jnp.sum(h_state, axis=1)
        w_colsum = jnp.sum(w_state, axis=0)

        def one_block(acc_h, block_in):
            count_blk, w_blk = block_in
            z_blk = jnp.dot(w_blk, h_bf, preferred_element_type=jnp.float32)
            q_blk = (count_blk.astype(jnp.float32) / z_blk).astype(jnp.bfloat16)
            num_w = jnp.dot(q_blk, h_bf.T, preferred_element_type=jnp.float32)
            acc_h = acc_h + jnp.dot(w_blk.T, q_blk, preferred_element_type=jnp.float32)
            return acc_h, num_w

        num_h, num_w = lax.scan(one_block, jnp.zeros((TOPICS, VOCAB), jnp.float32), (count_blocks, w_bf.reshape(num_blocks, BLOCK_ROWS, TOPICS)))
        w_next = w_state * num_w.reshape(DOCS, TOPICS) / h_rowsum[None, :]
        h_next = h_state * num_h / w_colsum[:, None]
        return (w_next, h_next), None

    final_state, unused = lax.scan(one_sweep, (w_init, h_init), None, length=SWEEPS)
    return final_state[0], final_state[1]
```

```python
import functools

import jax
import jax.numpy as jnp
from jax import lax
from jax.experimental import pallas as pl
from jax.experimental.pallas import tpu as pltpu
from jax.sharding import PartitionSpec as P

SWEEPS = 6
F32 = jnp.float32
BF16 = jnp.bfloat16
BV = 1024
VMEM = 60 * 1024 * 1024


def dot(a, b):
    return jnp.dot(a, b, preferred_element_type=F32)


def dot_t(a, b):
    return lax.dot_general(a, b, (((1,), (1,)), ((), ())), preferred_element_type=F32)


def ratio(c, z):
    return (c.astype(F32) / z).astype(BF16)


def lane_sum(h):
    out = h[:, :128]
    for g in range(1, h.shape[1] // 128):
        out = out + h[:, g * 128:(g + 1) * 128]
    return out


def first_kernel(row_ref, c_ref, wb_ref, wbt_ref, h_ref, nw_ref, nh_ref, hs_ref):
    j = pl.program_id(0)
    half = pl.num_programs(0) // 2

    @pl.when(j == 0)
    def _():
        nw_ref[...] = jnp.zeros_like(nw_ref)
        hs_ref[...] = jnp.zeros_like(hs_ref)

    hb = h_ref[...].astype(BF16)
    q = ratio(c_ref[...], dot(wb_ref[...], hb))
    nw_ref[...] += dot_t(q, hb)
    hs_ref[...] += lane_sum(h_ref[...])

    @pl.when(j < half)
    def _():
        nh_ref[...] = dot(wbt_ref[...], q)


def sweep_body(c_own, c_par, wb_ref, wbt_ref, ws, h, own, par, nw_ref, hs_ref):
    hb = h.astype(BF16)
    q_own = ratio(c_own[...], dot(wb_ref[own], hb))
    nw_ref[own] += dot_t(q_own, hb)
    nh = dot(wbt_ref[own], q_own)
    q_par = ratio(c_par[...], dot(wb_ref[par], hb))
    nw_ref[par] += dot_t(q_par, hb)
    nh = nh + dot(wbt_ref[par], q_par)
    new = h * nh / ws
    hs_ref[...] += lane_sum(new)
    return new


def chunk_kernel(row_ref, c_own, c_par, wb0_ref, wbt0_ref, ws0_ref, wb1_ref, wbt1_ref, ws1_ref, h_ref, nh_ref,
                 nw_in, hs1_in, hs2_in, h_out, nw_ref, hs1_ref, hs2_ref):
    own = row_ref[0]
    par = 1 - own
    nw_ref[...] = nw_in[...]
    hs1_ref[...] = hs1_in[...]
    hs2_ref[...] = hs2_in[...]
    h = h_ref[...]
    hb = h.astype(BF16)
    q = ratio(c_par[...], dot(wb0_ref[par], hb))
    nh = nh_ref[...] + dot(wbt0_ref[par], q)
    h = h * nh / ws0_ref[...]
    hs1_ref[...] += lane_sum(h)
    h_out[...] = sweep_body(c_own, c_par, wb1_ref, wbt1_ref, ws1_ref[...], h, own, par, nw_ref, hs2_ref)


def sweep_kernel(row_ref, c_own, c_par, wb_ref, wbt_ref, ws_ref, h_ref, h_out, nw_ref, hs_ref):
    own = row_ref[0]

    @pl.when(pl.program_id(0) == 0)
    def _():
        nw_ref[...] = jnp.zeros_like(nw_ref)
        hs_ref[...] = jnp.zeros_like(hs_ref)

    h_out[...] = sweep_body(c_own, c_par, wb_ref, wbt_ref, ws_ref[...], h_ref[...], own, 1 - own, nw_ref, hs_ref)


def params():
    return pltpu.CompilerParams(vmem_limit_bytes=VMEM, dimension_semantics=("arbitrary",))


def cost(docs, columns, topics, dots):
    return pl.CostEstimate(flops=int(2 * docs * columns * topics * dots), bytes_accessed=2 * docs * columns, transcendentals=0)


def whole(shape):
    return pl.BlockSpec(shape, lambda j, row: (0,) * len(shape))


def solution(mesh):
    rows, cols = mesh.shape["row"], mesh.shape["col"]

    def body(counts, w_own, h_blk):
        docs, width = counts.shape
        topics = w_own.shape[1]
        mine = width // rows
        blocks = mine // BV
        row = lax.axis_index("row")
        row_arr = row.astype(jnp.int32).reshape(1)
        swap = [(0, 1), (1, 0)]
        sds = jax.ShapeDtypeStruct
        lanes = (topics, 128)

        recv = []
        for j in range(blocks):
            piece = lax.dynamic_slice(counts, (0, (1 - row) * mine + j * BV), (docs, BV))
            recv.append(lax.ppermute(piece, "row", swap))

        w_all = lax.all_gather(w_own, "row")
        h_mine = lax.dynamic_slice(h_blk, (0, row * mine), (topics, mine))

        def forms(w):
            wb = w.astype(BF16)
            return wb, jnp.swapaxes(wb, 1, 2), jnp.sum(w, axis=(0, 1))[:, None]

        wb0, wbt0, ws0 = forms(w_all)
        wb_own = w_own.astype(BF16)

        def place(j, row):
            return jnp.where(j < blocks, row[0] * blocks + j, (1 - row[0]) * blocks + j - blocks)

        nw, nh1, hs0 = pl.pallas_call(
            first_kernel,
            grid_spec=pltpu.PrefetchScalarGridSpec(
                num_scalar_prefetch=1, grid=(rows * blocks,),
                in_specs=[
                    pl.BlockSpec((docs, BV), lambda j, row: (0, place(j, row))),
                    whole((docs, topics)), whole((topics, docs)),
                    pl.BlockSpec((topics, BV), lambda j, row: (0, place(j, row))),
                ],
                out_specs=[
                    whole((docs, topics)),
                    pl.BlockSpec((topics, BV), lambda j, row: (0, jnp.minimum(j, blocks - 1))),
                    whole(lanes),
                ]),
            out_shape=[sds((docs, topics), F32), sds((topics, mine), F32), sds(lanes, F32)],
            compiler_params=params(), cost_estimate=cost(docs, width, topics, 2.5), name="first",
        )(row_arr, counts, wb_own, wb_own.T, h_blk)

        def total(nw, hs):
            both = jnp.concatenate([nw.reshape(rows * docs, topics), jnp.tile(jnp.sum(hs, axis=1)[None, :], (8, 1))], axis=0)
            both = lax.psum(both, ("row", "col"))
            return both[:rows * docs].reshape(rows, docs, topics), both[rows * docs]

        nw_all = jnp.where(lax.broadcasted_iota(jnp.int32, (rows, 1, 1), 0) == row, nw[None], 0.0)
        nw_all, hs = total(nw_all, jnp.where(row == 0, hs0, 0.0))
        w = w_all * nw_all / hs[None, None, :]
        wb1, wbt1, ws1 = forms(w)

        nw = jnp.zeros((rows, docs, topics), F32)
        hs1 = jnp.zeros(lanes, F32)
        hs2 = jnp.zeros(lanes, F32)
        h_parts = []
        for j in range(blocks):
            h_new, nw, hs1, hs2 = pl.pallas_call(
                chunk_kernel,
                grid_spec=pltpu.PrefetchScalarGridSpec(
                    num_scalar_prefetch=1, grid=(1,),
                    in_specs=[
                        pl.BlockSpec((docs, BV), lambda i, row, j=j: (0, row[0] * blocks + j)),
                        whole((docs, BV)),
                        whole((rows, docs, topics)), whole((rows, topics, docs)), whole((topics, 1)),
                        whole((rows, docs, topics)), whole((rows, topics, docs)), whole((topics, 1)),
                        pl.BlockSpec((topics, BV), lambda i, row, j=j: (0, j)),
                        pl.BlockSpec((topics, BV), lambda i, row, j=j: (0, j)),
                        whole((rows, docs, topics)), whole(lanes), whole(lanes),
                    ],
                    out_specs=[whole((topics, BV)), whole((rows, docs, topics)), whole(lanes), whole(lanes)]),
                out_shape=[sds((topics, BV), F32), sds((rows, docs, topics), F32), sds(lanes, F32), sds(lanes, F32)],
                compiler_params=params(), cost_estimate=cost(docs, BV, topics, 8), name=f"chunk{j}",
            )(row_arr, counts, recv[j], wb0, wbt0, ws0, wb1, wbt1, ws1, h_mine, nh1, nw, hs1, hs2)
            h_parts.append(h_new)

        c_par = jnp.concatenate(recv, axis=1)
        h = jnp.concatenate(h_parts, axis=1)
        nw, hs = total(nw, hs1)
        w = w * nw / hs[None, None, :]
        hs_next = hs2

        def sweep(w, h, start, count):
            wb, wbt, ws = forms(w)
            return pl.pallas_call(
                sweep_kernel,
                grid_spec=pltpu.PrefetchScalarGridSpec(
                    num_scalar_prefetch=1, grid=(count,),
                    in_specs=[
                        pl.BlockSpec((docs, BV), lambda j, row: (0, row[0] * blocks + start + j)),
                        pl.BlockSpec((docs, BV), lambda j, row: (0, start + j)),
                        whole((rows, docs, topics)), whole((rows, topics, docs)), whole((topics, 1)),
                        pl.BlockSpec((topics, BV), lambda j, row: (0, start + j)),
                    ],
                    out_specs=[pl.BlockSpec((topics, BV), lambda j, row: (0, j)), whole((rows, docs, topics)), whole(lanes)]),
                out_shape=[sds((topics, count * BV), F32), sds((rows, docs, topics), F32), sds(lanes, F32)],
                compiler_params=params(), cost_estimate=cost(docs, count * BV, topics, 6), name="sweep",
            )(row_arr, counts, c_par, wb, wbt, ws, h)

        for sweep_idx in range(2, SWEEPS - 1):
            h, nw, hs_new = sweep(w, h, 0, blocks)
            nw, hs = total(nw, hs_next)
            w = w * nw / hs[None, None, :]
            hs_next = hs_new

        step = 2
        nw_sum = jnp.zeros((rows, docs, topics), F32)
        h_out = jnp.zeros((topics, width), F32)
        for start in range(0, blocks, step):
            h_piece, nw, _ = sweep(w, h, start, step)
            nw_sum = nw_sum + nw
            other = lax.ppermute(h_piece, "row", swap)
            h_out = lax.dynamic_update_slice(h_out, h_piece, (0, row * mine + start * BV))
            h_out = lax.dynamic_update_slice(h_out, other, (0, (1 - row) * mine + start * BV))
        nw, hs = total(nw_sum, hs_next)
        w = w * nw / hs[None, None, :]
        w_out = lax.dynamic_slice(w, (row, 0, 0), (1, docs, topics))[0]
        return w_out, h_out

    return jax.shard_map(
        body,
        mesh=mesh,
        in_specs=(P(("part", "row"), "col"), P(("part", "row"), None), P("part", "col")),
        out_specs=(P(("part", "row"), None), P("part", "col")),
        check_vma=False,
    )
```

```python
import functools

import jax
import jax.numpy as jnp
from jax import lax
from jax.experimental import pallas as pl
from jax.experimental.pallas import tpu as pltpu
from jax.sharding import PartitionSpec as P

SWEEPS = 6
F32 = jnp.float32
BF16 = jnp.bfloat16
BV = 1024
VMEM = 60 * 1024 * 1024


def dot(a, b):
    return jnp.dot(a, b, preferred_element_type=F32)


def dot_t(a, b):
    return lax.dot_general(a, b, (((1,), (1,)), ((), ())), preferred_element_type=F32)


def ratio(c, z):
    return (c.astype(F32) / z).astype(BF16)


def lane_sum(h):
    out = h[:, :128]
    for g in range(1, h.shape[1] // 128):
        out = out + h[:, g * 128:(g + 1) * 128]
    return out


def sweep_body(c_own, c_par, wb_ref, wbt_ref, ws, h, own, par, nw_ref, hs_ref):
    hb = h.astype(BF16)
    q_own = ratio(c_own[...], dot(wb_ref[own], hb))
    nw_ref[own] += dot_t(q_own, hb)
    nh = dot(wbt_ref[own], q_own)
    q_par = ratio(c_par[...], dot(wb_ref[par], hb))
    nw_ref[par] += dot_t(q_par, hb)
    nh = nh + dot(wbt_ref[par], q_par)
    new = h * nh / ws
    hs_ref[...] += lane_sum(new)
    return new


def sweep_kernel(row_ref, c_own, c_par, wb_ref, wbt_ref, ws_ref, h_ref, h_out, nw_ref, hs_ref):
    own = row_ref[0]

    @pl.when(pl.program_id(0) == 0)
    def _():
        nw_ref[...] = jnp.zeros_like(nw_ref)
        hs_ref[...] = jnp.zeros_like(hs_ref)

    h_out[...] = sweep_body(c_own, c_par, wb_ref, wbt_ref, ws_ref[...], h_ref[...], own, 1 - own, nw_ref, hs_ref)

DEVICES = 8
EXTRA = 8
CHUNK = 512
AHEAD = 6
UPDATE_AT = 3


def main_kernel(sweeps, grid_cols, counts, w_in, h_in,
                c_par, h_ref, wb_ref, ws_ref, hs_acc, wsl_ref,
                cbuf, hbuf, nh_ref, wbt_ref, wb0, wbt0, ws0_buf, ws0_ref, hs_first, acc, nw_recv, ws_buf, ws_half, hs_row,
                csem, psem, hsem, hhsem, c_send, c_got, w0_send, w0_got,
                nw_send, nw_got, wb_send, wb_got, ws_send, ws_got):
    row, col = lax.axis_index("row"), lax.axis_index("col")
    me = row * grid_cols + col
    docs, full = counts.shape
    topics, width = h_ref.shape
    blocks = width // BV
    chunks = width // CHUNK
    part = docs // DEVICES
    partner = {"row": 1 - row, "col": col}
    mesh_id = pl.DeviceIdType.MESH

    def remote(src, dst, send, got, where):
        return pltpu.make_async_remote_copy(src, dst, send, got, device_id=where, device_id_type=mesh_id)

    def peer(p):
        other = lax.rem(me + p, DEVICES)
        return {"row": other // grid_cols, "col": lax.rem(other, grid_cols)}, other

    def nw_copy(p, half):
        where, other = peer(p)
        return remote(acc.at[half, other], nw_recv.at[half, p], nw_send.at[half, p], nw_got.at[half, p], where)

    def wb_copy(p, half):
        mine = wb_ref.at[half, pl.ds(pl.multiple_of(me * part, part), part)]
        return remote(mine, mine, wb_send.at[half, p], wb_got.at[half, p], peer(p)[0])

    def ws_copy(p, half):
        return remote(ws_buf.at[half, 0], ws_buf.at[half, p], ws_send.at[half, p], ws_got.at[half, p], peer(p)[0])

    def first_copy(q, cross):
        to_row_, to_col = (1 - row if cross else row), lax.rem(col + q, grid_cols)
        slot = int(cross)
        return remote(acc.at[row, to_row_ * grid_cols + to_col], nw_recv.at[row, q], nw_send.at[slot, q],
                      nw_got.at[row, q], {"row": to_row_, "col": to_col})

    def first_arrival(q, half):
        return remote(acc.at[0, 0], nw_recv.at[half, q], nw_send.at[0, q], nw_got.at[half, q], partner)

    def chunk_copy(j):
        theirs = pl.ds(pl.multiple_of((1 - row) * width + j * CHUNK, CHUNK), CHUNK)
        here = pl.ds(pl.multiple_of(j * CHUNK, CHUNK), CHUNK)
        return remote(counts.at[:, theirs], c_par.at[:, here], c_send.at[j], c_got.at[j], partner)

    def w0_copies():
        other = (1 - row) * grid_cols + col
        return [
            remote(wb0.at[0], wb0.at[1], w0_send.at[0], w0_got.at[0], partner),
            remote(ws0_buf.at[0], ws0_buf.at[1], w0_send.at[1], w0_got.at[1], partner),
            remote(w_in.at[pl.ds(pl.multiple_of(other * part, part), part)], wsl_ref.at[row], w0_send.at[2], w0_got.at[2],
                   partner),
        ]

    def local(src, dst, sem):
        return pltpu.make_async_copy(src, dst, sem)

    def c_start(half, j, slot):
        @pl.when(row == half)
        def _():
            local(counts.at[:, pl.ds(pl.multiple_of(row * width + j * BV, BV), BV)], cbuf.at[slot], csem.at[slot]).start()

        @pl.when(row != half)
        def _():
            local(c_par.at[:, pl.ds(pl.multiple_of(j * BV, BV), BV)], cbuf.at[slot], csem.at[slot]).start()

    def c_wait(slot):
        local(counts.at[:, pl.ds(0, BV)], cbuf.at[slot], csem.at[slot]).wait()

    def first_c(i, slot):
        block = lax.rem(row * blocks + i, 2 * blocks)
        return local(counts.at[:, pl.ds(pl.multiple_of(block * BV, BV), BV)], cbuf.at[slot], csem.at[slot])

    def first_h(j, slot):
        at = pl.ds(pl.multiple_of((1 - row) * width + j * BV, BV), BV)
        return local(h_in.at[:, at], hbuf.at[slot], hsem.at[slot])

    def own_chunk(j, slot):
        at = pl.ds(pl.multiple_of(row * width + j * CHUNK, CHUNK), CHUNK)
        return local(counts.at[:, at], cbuf.at[slot, :, pl.ds(0, CHUNK)], csem.at[slot])

    def par_chunk(j, slot):
        at = pl.ds(pl.multiple_of(j * CHUNK, CHUNK), CHUNK)
        return local(c_par.at[:, at], cbuf.at[slot, :, pl.ds(CHUNK, CHUNK)], psem)

    def acc_add(half, res):
        for b in range(DEVICES):
            acc[half, b, pl.ds(0, part)] += res[b * part:(b + 1) * part]

    def acc_sums(half):
        for b in range(DEVICES):
            acc[half, b, pl.ds(part, EXTRA)] = hs_row[...]

    def acc_zero(half):
        acc[half] = jnp.zeros(acc.shape[1:], F32)

    def send_nw(half):
        acc_sums(half)
        for p in range(1, DEVICES):
            nw_copy(p, half).start()

    def publish(half, total):
        new = wsl_ref[half] * total[:part] / total[part:part + 1]
        wsl_ref[half] = new
        wb_ref[half, pl.ds(pl.multiple_of(me * part, part), part)] = new.astype(BF16)
        ws_buf[half, 0] = jnp.broadcast_to(jnp.sum(new, axis=0, keepdims=True), (EXTRA, topics))
        for p in range(1, DEVICES):
            wb_copy(p, half).start()
            ws_copy(p, half).start()

    def sent_w(half):
        for p in range(1, DEVICES):
            wb_copy(p, half).wait_send()
            ws_copy(p, half).wait_send()

    def sent_nw(half):
        for p in range(1, DEVICES):
            nw_copy(p, half).wait_send()

    def owner_update(half):
        for p in range(1, DEVICES):
            nw_copy(p, half).wait_recv()
        total = acc[half, me]
        for p in range(1, DEVICES):
            total = total + nw_recv[half, p]
        sent_w(half)
        publish(half, total)

    def receive_w(half):
        for p in range(1, DEVICES):
            wb_copy(p, half).wait_recv()
            ws_copy(p, half).wait_recv()
        wbt_ref[half] = wb_ref[half].T
        total = ws_buf[half, 0]
        for p in range(1, DEVICES):
            total = total + ws_buf[half, p]
        return total

    def to_row(lanes):
        return jnp.broadcast_to(jnp.sum(lanes.T, axis=0, keepdims=True), (EXTRA, topics))

    def to_lanes(sums):
        return jnp.broadcast_to(sums[:1], (128, topics)).T

    barrier = pltpu.get_barrier_semaphore()
    for p in range(1, DEVICES):
        pl.semaphore_signal(barrier, inc=1, device_id=peer(p)[0], device_id_type=mesh_id)

    own_h = local(h_in.at[:, pl.ds(pl.multiple_of(row * width, width), width)], h_ref, hhsem)
    own_h.start()
    first_c(0, 0).start()
    wb0[0] = w_in[...].astype(BF16)
    ws0_buf[0] = jnp.broadcast_to(jnp.sum(w_in[...], axis=0, keepdims=True), (EXTRA, topics))
    wsl_ref[row] = w_in[pl.ds(pl.multiple_of(me * part, part), part)]
    pl.semaphore_wait(barrier, DEVICES - 1)
    for copy in w0_copies():
        copy.start()
    for j in range(AHEAD):
        chunk_copy(j).start()
    wbt0[0] = wb0[0].T
    acc_zero(0)
    acc_zero(1)
    hs_first[...] = jnp.zeros_like(hs_first)
    hs_acc[...] = jnp.zeros_like(hs_acc)
    own_h.wait()

    def first_own(j, carry):
        slot = lax.rem(j, 2)
        first_c(j, slot).wait()
        first_c(j + 1, 1 - slot).start()

        @pl.when(j == blocks - 1)
        def _():
            first_h(0, 0).start()

        at = pl.ds(pl.multiple_of(j * BV, BV), BV)
        h = h_ref[:, at]
        hb = h.astype(BF16)
        q = ratio(cbuf[slot], dot(wb0[0], hb))
        acc_add(row, dot_t(q, hb))
        nh_ref[:, at] = dot(wbt0[0], q)
        hs_first[...] += lane_sum(h)
        return carry

    lax.fori_loop(0, blocks, first_own, 0)

    def first_other(j, carry):
        slot = lax.rem(j, 2)
        first_c(blocks + j, slot).wait()
        first_h(j, slot).wait()

        @pl.when(j < blocks - 1)
        def _():
            first_c(blocks + j + 1, 1 - slot).start()
            first_h(j + 1, 1 - slot).start()

        h = hbuf[slot]
        hb = h.astype(BF16)
        q = ratio(cbuf[slot], dot(wb0[0], hb))
        acc_add(row, dot_t(q, hb))
        hs_first[...] += lane_sum(h)
        return carry

    lax.fori_loop(0, blocks, first_other, 0)

    hs_row[...] = to_row(hs_first[...])
    acc_sums(row)
    for q in range(grid_cols):
        first_copy(q, True).start()
        if q:
            first_copy(q, False).start()
    own_chunk(0, 0).start()
    for copy in w0_copies():
        copy.wait_recv()
    wbt0[1] = wb0[1].T
    ws0_ref[...] = to_lanes(ws0_buf[0] + ws0_buf[1])
    hs_first[...] = jnp.zeros_like(hs_first)
    total = acc[row, me]
    for q in range(1, grid_cols):
        first_arrival(q, row).wait_recv()
        total = total + nw_recv[row, q]
    publish(row, total)
    first_arrival(0, 1 - row).wait_recv()
    total = nw_recv[1 - row, 0]
    for q in range(1, grid_cols):
        first_arrival(q, 1 - row).wait_recv()
        total = total + nw_recv[1 - row, q]
    publish(1 - row, total)
    for q in range(grid_cols):
        first_copy(q, True).wait_send()
        if q:
            first_copy(q, False).wait_send()
    acc_zero(row)
    ws_ref[...] = to_lanes(receive_w(0) + receive_w(1))

    def chunk_step(j, carry):
        slot = lax.rem(j, 2)
        chunk_copy(j).wait_recv()
        par_chunk(j, slot).start()
        chunk_copy(j).wait_send()

        @pl.when(jnp.logical_and(j >= AHEAD - 2, j < chunks - 2))
        def _():
            chunk_copy(j + 2).start()

        own_chunk(j, slot).wait()

        @pl.when(j < chunks - 1)
        def _():
            own_chunk(j + 1, 1 - slot).start()

        at = pl.ds(pl.multiple_of(j * CHUNK, CHUNK), CHUNK)
        h = h_ref[:, at]
        par_chunk(j, slot).wait()
        other = cbuf[slot, :, pl.ds(CHUNK, CHUNK)]
        q = ratio(other, dot(wb0[1], h.astype(BF16)))
        h = h * (nh_ref[:, at] + dot(wbt0[1], q)) / ws0_ref[:, :1]
        hs_first[...] += lane_sum(h)
        hb = h.astype(BF16)
        q = ratio(cbuf[slot, :, pl.ds(0, CHUNK)], dot(wb_ref[row], hb))
        acc_add(row, dot_t(q, hb))
        nh = dot(wbt_ref[row], q)
        q = ratio(other, dot(wb_ref[1 - row], hb))
        acc_add(1 - row, dot_t(q, hb))
        nh = nh + dot(wbt_ref[1 - row], q)
        h = h * nh / ws_ref[:, :1]
        h_ref[:, at] = h
        hs_acc[...] += lane_sum(h)
        return carry

    lax.fori_loop(0, chunks, chunk_step, 0)
    for copy in w0_copies():
        copy.wait_send()
    hs_row[...] = to_row(hs_first[...])
    send_nw(0)
    send_nw(1)
    c_start(0, 0, 0)
    owner_update(0)

    def step(half, j, last):
        slot = lax.rem(j, 2)
        c_wait(slot)

        @pl.when(j < blocks - 1)
        def _():
            c_start(half, j + 1, 1 - slot)

        @pl.when(jnp.logical_and(j == blocks - 1, jnp.logical_not(last)))
        def _():
            c_start(1 - half, 0, 1 - slot)

        at = pl.ds(pl.multiple_of(j * BV, BV), BV)
        hb = h_ref[:, at].astype(BF16)
        q = ratio(cbuf[slot], dot(wb_ref[half], hb))
        acc_add(half, dot_t(q, hb))
        nh = dot(wbt_ref[half], q)
        if half == 0:
            nh_ref[:, at] = nh
        else:
            new = h_ref[:, at] * (nh_ref[:, at] + nh) / ws_ref[:, :1]
            h_ref[:, at] = new
            hs_acc[...] += lane_sum(new)

    def one_sweep(s, carry):
        last = s == sweeps - 1
        ws_half[...] = receive_w(0)
        hs_row[...] = to_row(hs_acc[...])
        hs_acc[...] = jnp.zeros_like(hs_acc)
        sent_nw(0)
        acc_zero(0)

        def step_a(j, carry):
            @pl.when(j == UPDATE_AT)
            def _():
                owner_update(1)

            step(0, j, False)
            return carry

        lax.fori_loop(0, blocks, step_a, 0)
        send_nw(0)
        ws_ref[...] = to_lanes(ws_half[...] + receive_w(1))
        sent_nw(1)
        acc_zero(1)

        def step_b(j, carry):
            @pl.when(j == UPDATE_AT)
            def _():
                owner_update(0)

            step(1, j, last)
            return carry

        lax.fori_loop(0, blocks, step_b, 0)
        send_nw(1)
        return carry

    lax.fori_loop(0, sweeps, one_sweep, 0)
    owner_update(1)
    ws_ref[...] = to_lanes(receive_w(0) + receive_w(1))
    for half in range(2):
        sent_nw(half)
        sent_w(half)


def params():
    return pltpu.CompilerParams(vmem_limit_bytes=VMEM, dimension_semantics=("arbitrary",))


def cost(docs, columns, topics, dots):
    return pl.CostEstimate(flops=int(2 * docs * columns * topics * dots), bytes_accessed=2 * docs * columns, transcendentals=0)


def whole(shape):
    return pl.BlockSpec(shape, lambda j, row: (0,) * len(shape))


def solution(mesh):
    rows, cols = mesh.shape["row"], mesh.shape["col"]

    def body(counts, w_own, h_blk):
        docs, width = counts.shape
        topics = w_own.shape[1]
        mine = width // rows
        blocks = mine // BV
        row = lax.axis_index("row")
        row_arr = row.astype(jnp.int32).reshape(1)
        swap = [(0, 1), (1, 0)]
        sds = jax.ShapeDtypeStruct
        lanes = (topics, 128)

        def total(nw, hs):
            both = jnp.concatenate([nw.reshape(rows * docs, topics), jnp.tile(jnp.sum(hs, axis=1)[None, :], (8, 1))], axis=0)
            both = lax.psum(both, ("row", "col"))
            return both[:rows * docs].reshape(rows, docs, topics), both[rows * docs]

        part = docs // DEVICES
        me = row * cols + lax.axis_index("col")
        vmem, hbm = pl.BlockSpec(memory_space=pltpu.VMEM), pl.BlockSpec(memory_space=pl.ANY)
        dma = pltpu.SemaphoreType.DMA
        V = pltpu.VMEM
        exchange = V((rows, DEVICES, part + EXTRA, topics), F32)
        c_par, h, wb, ws, hs_next, wsl = pl.pallas_call(
            functools.partial(main_kernel, SWEEPS - 3, cols),
            in_specs=[hbm, vmem, hbm],
            out_specs=[hbm] + [vmem] * 5,
            out_shape=[sds((docs, mine), BF16), sds((topics, mine), F32), sds((rows, docs, topics), BF16), sds(lanes, F32),
                       sds(lanes, F32), sds((rows, part, topics), F32)],
            scratch_shapes=[
                V((2, docs, BV), BF16), V((2, topics, BV), F32), V((topics, mine), F32), V((rows, topics, docs), BF16),
                V((2, docs, topics), BF16), V((2, topics, docs), BF16), V((2, EXTRA, topics), F32), V(lanes, F32),
                V(lanes, F32), exchange, exchange, V((rows, DEVICES, EXTRA, topics), F32),
                V((EXTRA, topics), F32), V((EXTRA, topics), F32),
                dma((2,)), dma, dma((2,)), dma, dma((mine // CHUNK,)), dma((mine // CHUNK,)), dma((3,)), dma((3,)),
            ] + [dma((rows, DEVICES))] * 6,
            compiler_params=pltpu.CompilerParams(vmem_limit_bytes=VMEM, collective_id=0, has_side_effects=True),
            cost_estimate=cost(rows * docs, mine, topics, 15), name="main",
        )(counts, w_own, h_blk)
        wbt = jnp.swapaxes(wb, 1, 2)
        ws = ws[:, :1]

        step = 2
        nw_sum = jnp.zeros((rows, docs, topics), F32)
        h_out = jnp.zeros((topics, width), F32)
        for start in range(0, blocks, step):
            with jax.named_scope(f"piece{start}"):
                h_piece, nw, _ = pl.pallas_call(
                    sweep_kernel,
                    grid_spec=pltpu.PrefetchScalarGridSpec(
                        num_scalar_prefetch=1, grid=(step,),
                        in_specs=[
                            pl.BlockSpec((docs, BV), lambda j, row: (0, row[0] * blocks + start + j)),
                            pl.BlockSpec((docs, BV), lambda j, row: (0, start + j)),
                            whole((rows, docs, topics)), whole((rows, topics, docs)), whole((topics, 1)),
                            pl.BlockSpec((topics, BV), lambda j, row: (0, start + j)),
                        ],
                        out_specs=[pl.BlockSpec((topics, BV), lambda j, row: (0, j)), whole((rows, docs, topics)), whole(lanes)]),
                    out_shape=[sds((topics, step * BV), F32), sds((rows, docs, topics), F32), sds(lanes, F32)],
                    compiler_params=params(), cost_estimate=cost(docs, step * BV, topics, 6), name="sweep",
                )(row_arr, counts, c_par, wb, wbt, ws, h)
            nw_sum = nw_sum + nw
            with jax.named_scope(f"send{start}"):
                other = lax.ppermute(h_piece, "row", swap)
            h_out = lax.dynamic_update_slice(h_out, h_piece, (0, row * mine + start * BV))
            h_out = lax.dynamic_update_slice(h_out, other, (0, (1 - row) * mine + start * BV))
        nw, hs = total(nw_sum, hs_next)
        slices = lambda a: lax.dynamic_slice(a, (0, me * part, 0), (rows, part, topics))
        wsl = wsl * slices(nw) / hs[None, None, :]
        w_all = lax.all_gather(wsl, ("row", "col"))
        w_out = lax.dynamic_slice(w_all, (0, row, 0, 0), (DEVICES, 1, part, topics)).reshape(docs, topics)
        return w_out, h_out

    return jax.shard_map(
        body,
        mesh=mesh,
        in_specs=(P(("part", "row"), "col"), P(("part", "row"), None), P("part", "col")),
        out_specs=(P(("part", "row"), None), P("part", "col")),
        check_vma=False,
    )
```

```python
import functools

import jax
import jax.numpy as jnp
from jax import lax
from jax.experimental import pallas as pl
from jax.experimental.pallas import tpu as pltpu
from jax.sharding import PartitionSpec as P

SWEEPS = 6
F32 = jnp.float32
BF16 = jnp.bfloat16
BV = 1024
VMEM = 60 * 1024 * 1024


def dot(a, b):
    return jnp.dot(a, b, preferred_element_type=F32)


def dot_t(a, b):
    return lax.dot_general(a, b, (((1,), (1,)), ((), ())), preferred_element_type=F32)


def ratio(c, z):
    return (c.astype(F32) / z).astype(BF16)


def lane_sum(h):
    out = h[:, :128]
    for g in range(1, h.shape[1] // 128):
        out = out + h[:, g * 128:(g + 1) * 128]
    return out


DEVICES = 8
EXTRA = 8
CHUNK = 512
AHEAD = 4
UPDATE_AT = 4


def main_kernel(sweeps, grid_cols, counts, w_in, h_in,
                c_par, h_pair, h_last, w_out,
                h_ref, wb_ref, ws_ref, hs_acc, wsl_ref, wfin, cbuf, hbuf, nh_ref, wbt_ref, wb0, wbt0, ws0_buf, ws0_ref, hs_first, acc, nw_recv, ws_buf, ws_half, hs_row,
                csem, psem, hsem, hhsem, c_send, c_got, w0_send, w0_got,
                nw_send, nw_got, wb_send, wb_got, ws_send, ws_got,
                h_send, h_got, out_sem, wf_send, wf_got, fin_send, fin_got):
    row, col = lax.axis_index("row"), lax.axis_index("col")
    me = row * grid_cols + col
    docs, full = counts.shape
    topics, width = h_ref.shape
    blocks = width // BV
    chunks = width // CHUNK
    part = docs // DEVICES
    partner = {"row": 1 - row, "col": col}
    mesh_id = pl.DeviceIdType.MESH

    def remote(src, dst, send, got, where):
        return pltpu.make_async_remote_copy(src, dst, send, got, device_id=where, device_id_type=mesh_id)

    def peer(p):
        other = lax.rem(me + p, DEVICES)
        return {"row": other // grid_cols, "col": lax.rem(other, grid_cols)}, other

    def nw_copy(p, half):
        where, other = peer(p)
        return remote(acc.at[half, other], nw_recv.at[half, p], nw_send.at[half, p], nw_got.at[half, p], where)

    def wb_copy(p, half):
        mine = wb_ref.at[half, pl.ds(pl.multiple_of(me * part, part), part)]
        return remote(mine, mine, wb_send.at[half, p], wb_got.at[half, p], peer(p)[0])

    def ws_copy(p, half):
        return remote(ws_buf.at[half, 0], ws_buf.at[half, p], ws_send.at[half, p], ws_got.at[half, p], peer(p)[0])

    def row_peer(q):
        there = lax.rem(col + q, grid_cols)
        return {"row": row, "col": there}, there

    def first_copy(q):
        where, there = row_peer(q)
        return remote(acc.at[row, pl.ds(2 * there, 2)], nw_recv.at[row, pl.ds(2 * q, 2)], fin_send.at[q], fin_got.at[q], where)

    def first_wb(half, q):
        where = row_peer(q)[0] if q else partner
        mine = wb_ref.at[half, pl.ds(pl.multiple_of(col * 2 * part, 2 * part), 2 * part)]
        return remote(mine, mine, wb_send.at[half, q], wb_got.at[half, q], where)

    def first_ws(half, q):
        where = row_peer(q)[0] if q else partner
        return remote(ws_buf.at[half, 0], ws_buf.at[half, q], ws_send.at[half, q], ws_got.at[half, q], where)

    def first_owner(b):
        d = 2 * col + b
        return remote(wfin.at[b], wsl_ref.at[row], wf_send.at[b], wf_got.at[row],
                      {"row": d // grid_cols, "col": lax.rem(d, grid_cols)})

    def chunk_copy(j):
        theirs = pl.ds(pl.multiple_of((1 - row) * width + j * CHUNK, CHUNK), CHUNK)
        here = pl.ds(pl.multiple_of(j * CHUNK, CHUNK), CHUNK)
        return remote(counts.at[:, theirs], c_par.at[:, here], c_send.at[j], c_got.at[j], partner)

    half_docs = docs // 2

    def w0_part(of_core):
        return pl.ds(pl.multiple_of(of_core * half_docs, half_docs), half_docs)

    core = lax.rem(col, 2)

    def w0_copies():
        at = w0_part(core)
        return [
            remote(wb0.at[0, at], wb0.at[1, at], w0_send.at[0], w0_got.at[0], partner),
            remote(ws0_buf.at[0], ws0_buf.at[1], w0_send.at[1], w0_got.at[1], partner),
        ]

    def w0_forward():
        at = w0_part(core)
        return remote(wb0.at[1, at], wb0.at[1, at], w0_send.at[2], w0_got.at[2], {"row": row, "col": col + 1 - 2 * core})

    def local(src, dst, sem):
        return pltpu.make_async_copy(src, dst, sem)

    def c_start(half, j, slot):
        @pl.when(row == half)
        def _():
            local(counts.at[:, pl.ds(pl.multiple_of(row * width + j * BV, BV), BV)], cbuf.at[slot], csem.at[slot]).start()

        @pl.when(row != half)
        def _():
            local(c_par.at[:, pl.ds(pl.multiple_of(j * BV, BV), BV)], cbuf.at[slot], csem.at[slot]).start()

    def c_wait(slot):
        local(counts.at[:, pl.ds(0, BV)], cbuf.at[slot], csem.at[slot]).wait()

    def first_c(i, slot):
        block = lax.rem(row * blocks + i, 2 * blocks)
        return local(counts.at[:, pl.ds(pl.multiple_of(block * BV, BV), BV)], cbuf.at[slot], csem.at[slot])

    def first_h(j, slot):
        at = pl.ds(pl.multiple_of((1 - row) * width + j * BV, BV), BV)
        return local(h_in.at[:, at], hbuf.at[slot], hsem.at[slot])

    def own_chunk(j, slot):
        at = pl.ds(pl.multiple_of(row * width + j * CHUNK, CHUNK), CHUNK)
        return local(counts.at[:, at], cbuf.at[slot, :, pl.ds(0, CHUNK)], csem.at[slot])

    def par_chunk(j, slot):
        at = pl.ds(pl.multiple_of(j * CHUNK, CHUNK), CHUNK)
        return local(c_par.at[:, at], cbuf.at[slot, :, pl.ds(CHUNK, CHUNK)], psem.at[slot])

    def acc_add(half, res):
        for b in range(DEVICES):
            acc[half, b, pl.ds(0, part)] += res[b * part:(b + 1) * part]

    def acc_sums(half):
        for b in range(DEVICES):
            acc[half, b, pl.ds(part, EXTRA)] = hs_row[...]

    def acc_zero(half):
        acc[half] = jnp.zeros(acc.shape[1:], F32)

    def send_nw(half):
        acc_sums(half)
        for p in range(1, DEVICES):
            nw_copy(p, half).start()

    def publish(half, total):
        new = wsl_ref[half] * total[:part] / total[part:part + 1]
        wsl_ref[half] = new
        wb_ref[half, pl.ds(pl.multiple_of(me * part, part), part)] = new.astype(BF16)
        ws_buf[half, 0] = jnp.broadcast_to(jnp.sum(new, axis=0, keepdims=True), (EXTRA, topics))
        for p in range(1, DEVICES):
            wb_copy(p, half).start()
            ws_copy(p, half).start()

    def sent_w(half):
        for p in range(1, DEVICES):
            wb_copy(p, half).wait_send()
            ws_copy(p, half).wait_send()

    def sent_nw(half):
        for p in range(1, DEVICES):
            nw_copy(p, half).wait_send()

    def owner_update(half):
        for p in range(1, DEVICES):
            nw_copy(p, half).wait_recv()
        total = acc[half, me]
        for p in range(1, DEVICES):
            total = total + nw_recv[half, p]
        publish(half, total)

    def receive_w(half):
        for p in range(1, DEVICES):
            wb_copy(p, half).wait_recv()
            ws_copy(p, half).wait_recv()
        wbt_ref[half] = wb_ref[half].T
        total = ws_buf[half, 0]
        for p in range(1, DEVICES):
            total = total + ws_buf[half, p]
        return total

    def wfin_copy(half):
        return remote(wsl_ref.at[half], wfin.at[lax.rem(me, 2)], wf_send.at[half], wf_got.at[lax.rem(me, 2)],
                      {"row": jnp.int32(half), "col": me // 2})

    def wfin_here(half):
        return jnp.logical_and(row == half, col == me // 2)

    def fin_copy(q):
        there = lax.rem(col + q, grid_cols)
        return remote(acc.at[:, pl.ds(2 * there, 2)], nw_recv.at[:, pl.ds(2 * q, 2)], fin_send.at[q], fin_got.at[q],
                      {"row": row, "col": there})

    def fin_cross():
        pair = nw_recv.at[1 - row, pl.ds(0, 2)]
        return remote(pair, pair, fin_send.at[0], fin_got.at[0], partner)

    def out_copy(q):
        mine = w_out.at[pl.ds(pl.multiple_of(col * 2 * part, 2 * part), 2 * part)]
        return remote(mine, mine, fin_send.at[grid_cols + q], fin_got.at[grid_cols + q],
                      {"row": row, "col": lax.rem(col + q, grid_cols)})

    def h_remote(j):
        at = pl.ds(pl.multiple_of(j * CHUNK, CHUNK), CHUNK)
        return remote(h_ref.at[:, at], h_pair.at[row, :, at], h_send.at[j], h_got.at[j], partner)

    def h_local(j):
        at = pl.ds(pl.multiple_of(j * CHUNK, CHUNK), CHUNK)
        return local(h_ref.at[:, at], h_pair.at[row, :, at], out_sem.at[j])

    def to_row(lanes):
        return jnp.broadcast_to(jnp.sum(lanes.T, axis=0, keepdims=True), (EXTRA, topics))

    def to_lanes(sums):
        return jnp.broadcast_to(sums[:1], (128, topics)).T

    barrier = pltpu.get_barrier_semaphore()
    for p in range(1, DEVICES):
        pl.semaphore_signal(barrier, inc=1, device_id=peer(p)[0], device_id_type=mesh_id)

    own_h = local(h_in.at[:, pl.ds(pl.multiple_of(row * width, width), width)], h_ref, hhsem)
    own_h.start()
    first_c(0, 0).start()
    wb0[0] = w_in[...].astype(BF16)
    ws0_buf[0] = jnp.broadcast_to(jnp.sum(w_in[...], axis=0, keepdims=True), (EXTRA, topics))
    pl.semaphore_wait(barrier, DEVICES - 1)
    for copy in w0_copies():
        copy.start()
    for j in range(AHEAD):
        chunk_copy(j).start()
    wbt0[0] = wb0[0].T
    acc_zero(0)
    acc_zero(1)
    hs_first[...] = jnp.zeros_like(hs_first)
    hs_acc[...] = jnp.zeros_like(hs_acc)
    own_h.wait()

    def first_own(j, carry):
        slot = lax.rem(j, 2)
        first_c(j, slot).wait()
        first_c(j + 1, 1 - slot).start()

        @pl.when(j == blocks - 1)
        def _():
            first_h(0, 0).start()

        at = pl.ds(pl.multiple_of(j * BV, BV), BV)
        h = h_ref[:, at]
        hb = h.astype(BF16)
        q = ratio(cbuf[slot], dot(wb0[0], hb))
        acc_add(row, dot_t(q, hb))
        nh_ref[:, at] = dot(wbt0[0], q)
        hs_first[...] += lane_sum(h)
        return carry

    lax.fori_loop(0, blocks, first_own, 0)

    def first_other(j, carry):
        slot = lax.rem(j, 2)
        first_c(blocks + j, slot).wait()
        first_h(j, slot).wait()

        @pl.when(j < blocks - 1)
        def _():
            first_c(blocks + j + 1, 1 - slot).start()
            first_h(j + 1, 1 - slot).start()

        h = hbuf[slot]
        hb = h.astype(BF16)
        q = ratio(cbuf[slot], dot(wb0[0], hb))
        acc_add(row, dot_t(q, hb))
        hs_first[...] += lane_sum(h)
        return carry

    lax.fori_loop(0, blocks, first_other, 0)

    hs_row[...] = to_row(hs_first[...])
    acc_sums(row)
    for q in range(1, grid_cols):
        first_copy(q).start()
    own_chunk(0, 0).start()
    for copy in w0_copies():
        copy.wait_recv()
    w0_forward().start()
    for q in range(1, grid_cols):
        first_copy(q).wait_recv()
    total = acc[row, pl.ds(2 * col, 2)]
    for q in range(1, grid_cols):
        total = total + nw_recv[row, pl.ds(2 * q, 2)]
    sums = jnp.zeros((1, topics), F32)
    for b in range(2):
        at = pl.ds(pl.multiple_of((2 * col + b) * part, part), part)
        new = w_in[at] * total[b, :part] / total[b, part:part + 1]
        wfin[b] = new
        wb_ref[row, at] = new.astype(BF16)
        sums = sums + jnp.sum(new, axis=0, keepdims=True)
    ws_buf[row, 0] = jnp.broadcast_to(sums, (EXTRA, topics))
    for q in range(grid_cols):
        first_wb(row, q).start()
        first_ws(row, q).start()
    for b in range(2):
        @pl.when(2 * col + b == me)
        def _():
            wsl_ref[row] = wfin[b]

        @pl.when(2 * col + b != me)
        def _():
            first_owner(b).start()

    first_wb(1 - row, 0).wait_recv()
    first_ws(1 - row, 0).wait_recv()
    for q in range(1, grid_cols):
        first_wb(1 - row, q).start()
        first_ws(1 - row, q).start()
    w0_forward().wait_recv()
    wbt0[1] = wb0[1].T
    ws0_ref[...] = to_lanes(ws0_buf[0] + ws0_buf[1])
    hs_first[...] = jnp.zeros_like(hs_first)
    for q in range(1, grid_cols):
        first_copy(q).wait_send()
    acc_zero(row)
    total = ws_buf[0, 0] + ws_buf[1, 0]
    for half in range(2):
        for q in range(1, grid_cols):
            first_wb(half, q).wait_recv()
            first_ws(half, q).wait_recv()
            total = total + ws_buf[half, q]
        wbt_ref[half] = wb_ref[half].T
    ws_ref[...] = to_lanes(total)

    def both_halves(slot, h):
        hb = h.astype(BF16)
        q = ratio(cbuf[slot, :, pl.ds(0, CHUNK)], dot(wb_ref[row], hb))
        acc_add(row, dot_t(q, hb))
        nh = dot(wbt_ref[row], q)
        q = ratio(cbuf[slot, :, pl.ds(CHUNK, CHUNK)], dot(wb_ref[1 - row], hb))
        acc_add(1 - row, dot_t(q, hb))
        nh = nh + dot(wbt_ref[1 - row], q)
        return h * nh / ws_ref[:, :1]

    def chunk_step(j, carry):
        slot = lax.rem(j, 2)
        chunk_copy(j).wait_recv()
        par_chunk(j, slot).start()
        chunk_copy(j).wait_send()

        @pl.when(j < chunks // 2)
        def _():
            chunk_copy(j + AHEAD).start()

        @pl.when(jnp.logical_and(j >= chunks // 2 + AHEAD - 2, j < chunks - 2))
        def _():
            chunk_copy(j + 2).start()

        own_chunk(j, slot).wait()

        @pl.when(j < chunks - 1)
        def _():
            own_chunk(j + 1, 1 - slot).start()

        at = pl.ds(pl.multiple_of(j * CHUNK, CHUNK), CHUNK)
        h = h_ref[:, at]
        par_chunk(j, slot).wait()
        other = cbuf[slot, :, pl.ds(CHUNK, CHUNK)]
        q = ratio(other, dot(wb0[1], h.astype(BF16)))
        h = h * (nh_ref[:, at] + dot(wbt0[1], q)) / ws0_ref[:, :1]
        hs_first[...] += lane_sum(h)
        h = both_halves(slot, h)
        h_ref[:, at] = h
        hs_acc[...] += lane_sum(h)
        return carry

    lax.fori_loop(0, chunks, chunk_step, 0)
    for copy in w0_copies():
        copy.wait_send()
    w0_forward().wait_send()
    first_wb(row, 0).wait_send()
    first_ws(row, 0).wait_send()
    for half in range(2):
        for q in range(1, grid_cols):
            first_wb(half, q).wait_send()
            first_ws(half, q).wait_send()

        @pl.when(2 * col + half != me)
        def _():
            first_owner(half).wait_send()

        @pl.when(jnp.logical_not(wfin_here(half)))
        def _():
            remote(wfin.at[0], wsl_ref.at[half], wf_send.at[0], wf_got.at[half], partner).wait_recv()

    hs_row[...] = to_row(hs_first[...])
    send_nw(0)
    send_nw(1)
    c_start(0, 0, 0)
    owner_update(0)

    def step(half, j, last):
        slot = lax.rem(j, 2)
        c_wait(slot)

        @pl.when(j < blocks - 1)
        def _():
            c_start(half, j + 1, 1 - slot)

        @pl.when(jnp.logical_and(j == blocks - 1, jnp.logical_not(last)))
        def _():
            c_start(1 - half, 0, 1 - slot)

        at = pl.ds(pl.multiple_of(j * BV, BV), BV)
        hb = h_ref[:, at].astype(BF16)
        q = ratio(cbuf[slot], dot(wb_ref[half], hb))
        acc_add(half, dot_t(q, hb))
        nh = dot(wbt_ref[half], q)
        if half == 0:
            nh_ref[:, at] = nh
        else:
            new = h_ref[:, at] * (nh_ref[:, at] + nh) / ws_ref[:, :1]
            h_ref[:, at] = new
            hs_acc[...] += lane_sum(new)

    def one_sweep(s, carry):
        last = s == sweeps - 1
        ws_half[...] = receive_w(0)
        sent_w(0)
        hs_row[...] = to_row(hs_acc[...])
        hs_acc[...] = jnp.zeros_like(hs_acc)
        sent_nw(0)
        acc_zero(0)

        def step_a(j, carry):
            @pl.when(j == UPDATE_AT)
            def _():
                owner_update(1)

            step(0, j, False)
            return carry

        lax.fori_loop(0, blocks, step_a, 0)
        send_nw(0)
        ws_ref[...] = to_lanes(ws_half[...] + receive_w(1))
        sent_w(1)
        sent_nw(1)
        acc_zero(1)

        def step_b(j, carry):
            @pl.when(j == UPDATE_AT)
            def _():
                owner_update(0)

            step(1, j, last)
            return carry

        lax.fori_loop(0, blocks, step_b, 0)
        send_nw(1)
        return carry

    lax.fori_loop(0, sweeps, one_sweep, 0)
    own_chunk(0, 0).start()
    par_chunk(0, 0).start()
    owner_update(1)
    for half in range(2):
        @pl.when(wfin_here(half))
        def _():
            wfin[lax.rem(me, 2)] = wsl_ref[half]

        @pl.when(jnp.logical_not(wfin_here(half)))
        def _():
            wfin_copy(half).start()

    hs_row[...] = to_row(hs_acc[...])
    for half in range(2):
        sent_nw(half)
        acc_zero(half)
    ws_ref[...] = to_lanes(receive_w(0) + receive_w(1))

    def last_step(j, carry):
        slot = lax.rem(j, 2)
        own_chunk(j, slot).wait()
        par_chunk(j, slot).wait()

        @pl.when(j < chunks - 1)
        def _():
            own_chunk(j + 1, 1 - slot).start()
            par_chunk(j + 1, 1 - slot).start()

        @pl.when(j > 0)
        def _():
            h_remote(j - 1).start()
            h_local(j - 1).start()

        at = pl.ds(pl.multiple_of(j * CHUNK, CHUNK), CHUNK)
        h_ref[:, at] = both_halves(slot, h_ref[:, at])
        return carry

    lax.fori_loop(0, chunks, last_step, 0)
    for half in range(2):
        acc_sums(half)
    h_local(chunks - 1).start()
    tail = local(h_ref.at[:, pl.ds(width - CHUNK, CHUNK)], h_last, hhsem)
    tail.start()
    for q in range(1, grid_cols):
        fin_copy(q).start()
    for half in range(2):
        @pl.when(jnp.logical_not(wfin_here(half)))
        def _():
            wfin_copy(half).wait_send()

    for parity in range(2):
        @pl.when(2 * col + parity != me)
        def _():
            remote(wsl_ref.at[0], wfin.at[parity], wf_send.at[0], wf_got.at[parity], partner).wait_recv()

    for q in range(1, grid_cols):
        fin_copy(q).wait_recv()
    ours = acc[row, pl.ds(2 * col, 2)]
    theirs = acc[1 - row, pl.ds(2 * col, 2)]
    for q in range(1, grid_cols):
        ours = ours + nw_recv[row, pl.ds(2 * q, 2)]
        theirs = theirs + nw_recv[1 - row, pl.ds(2 * q, 2)]
    nw_recv[1 - row, pl.ds(0, 2)] = theirs
    fin_cross().start()
    fin_cross().wait_recv()
    total = ours + nw_recv[row, pl.ds(0, 2)]
    new = wfin[...] * total[:, :part] / total[:1, part:part + 1]
    for b in range(2):
        w_out[pl.ds(pl.multiple_of((2 * col + b) * part, part), part)] = new[b]
    for q in range(1, grid_cols):
        out_copy(q).start()
    for half in range(2):
        sent_w(half)
    for q in range(1, grid_cols):
        out_copy(q).wait()
        fin_copy(q).wait_send()
    fin_cross().wait_send()

    tail.wait()

    def drain(j, carry):
        h_remote(j).wait_recv()
        h_remote(j).wait_send()
        h_local(j).wait()
        return carry

    lax.fori_loop(0, chunks - 1, drain, 0)
    h_local(chunks - 1).wait()


PLACE = 2048


def place_kernel(h_pair, h_out, buf, in_sem, out_sem):
    row = lax.axis_index("row")
    width = h_pair.shape[2]
    jobs = []
    for other in range(2):
        half = 1 - row if other else row
        for start in range(0, width, PLACE):
            size = PLACE - CHUNK if other and start + PLACE == width else PLACE
            n = len(jobs)
            held = buf.at[n, :, pl.ds(0, size)]
            jobs.append((
                pltpu.make_async_copy(h_pair.at[half, :, pl.ds(start, size)], held, in_sem.at[n]),
                pltpu.make_async_copy(held, h_out.at[:, pl.ds(pl.multiple_of(half * width + start, PLACE), size)], out_sem.at[n]),
            ))
    for load, _ in jobs:
        load.start()
    for load, store in jobs:
        load.wait()
        store.start()
    for _, store in jobs:
        store.wait()


def cost(docs, columns, topics, dots):
    return pl.CostEstimate(flops=int(2 * docs * columns * topics * dots), bytes_accessed=2 * docs * columns, transcendentals=0)


def solution(mesh):
    rows, cols = mesh.shape["row"], mesh.shape["col"]

    def body(counts, w_own, h_blk):
        docs, width = counts.shape
        topics = w_own.shape[1]
        mine = width // rows
        sds = jax.ShapeDtypeStruct
        lanes = (topics, 128)
        part = docs // DEVICES
        vmem, hbm = pl.BlockSpec(memory_space=pltpu.VMEM), pl.BlockSpec(memory_space=pl.ANY)
        dma = pltpu.SemaphoreType.DMA
        V = pltpu.VMEM
        exchange = V((rows, DEVICES, part + EXTRA, topics), F32)
        pieces = mine // CHUNK
        c_par, h_pair, h_last, w_out = pl.pallas_call(
            functools.partial(main_kernel, SWEEPS - 3, cols),
            in_specs=[hbm, vmem, hbm],
            out_specs=[hbm, hbm, hbm, vmem],
            out_shape=[sds((docs, mine), BF16), sds((rows, topics, mine), F32), sds((topics, CHUNK), F32),
                       sds((docs, topics), F32)],
            scratch_shapes=[
                V((topics, mine), F32), V((rows, docs, topics), BF16), V(lanes, F32), V(lanes, F32),
                V((rows, part, topics), F32), V((2, part, topics), F32),
                V((2, docs, BV), BF16), V((2, topics, BV), F32), V((topics, mine), F32), V((rows, topics, docs), BF16),
                V((2, docs, topics), BF16), V((2, topics, docs), BF16), V((2, EXTRA, topics), F32), V(lanes, F32),
                V(lanes, F32), exchange, exchange, V((rows, DEVICES, EXTRA, topics), F32),
                V((EXTRA, topics), F32), V((EXTRA, topics), F32),
                dma((2,)), dma((2,)), dma((2,)), dma, dma((pieces,)), dma((pieces,)), dma((3,)), dma((3,)),
            ] + [dma((rows, DEVICES))] * 6 + [dma((pieces,))] * 3 + [dma((2,))] * 2 + [dma((2 * cols,))] * 2,
            compiler_params=pltpu.CompilerParams(vmem_limit_bytes=VMEM, collective_id=0, has_side_effects=True),
            cost_estimate=cost(rows * docs, mine, topics, 18), name="main",
        )(counts, w_own, h_blk)
        other = lax.ppermute(h_last, "row", [(0, 1), (1, 0)])
        row = lax.axis_index("row")
        jobs = 2 * mine // PLACE
        h_out = pl.pallas_call(
            place_kernel,
            in_specs=[hbm], out_specs=hbm, out_shape=sds((topics, width), F32),
            scratch_shapes=[V((jobs, topics, PLACE), F32), dma((jobs,)), dma((jobs,))],
            compiler_params=pltpu.CompilerParams(vmem_limit_bytes=VMEM),
            cost_estimate=pl.CostEstimate(flops=10 ** 8, bytes_accessed=8 * topics * width, transcendentals=0), name="place",
        )(h_pair)
        h_out = lax.dynamic_update_slice(h_out, other, (0, (1 - row) * mine + mine - CHUNK))
        return w_out, h_out

    return jax.shard_map(
        body,
        mesh=mesh,
        in_specs=(P(("part", "row"), "col"), P(("part", "row"), None), P("part", "col")),
        out_specs=(P(("part", "row"), None), P("part", "col")),
        check_vma=False,
    )
```

```python
import functools

import jax
import jax.numpy as jnp
from jax import lax
from jax.experimental import pallas as pl
from jax.experimental.pallas import tpu as pltpu
from jax.sharding import PartitionSpec as P

SWEEPS = 6
F32 = jnp.float32
BF16 = jnp.bfloat16
BV = 1024
VMEM = 60 * 1024 * 1024


def dot(a, b):
    return jnp.dot(a, b, preferred_element_type=F32)


def dot_t(a, b):
    return lax.dot_general(a, b, (((1,), (1,)), ((), ())), preferred_element_type=F32)


def ratio(c, z):
    return (c.astype(F32) / z).astype(BF16)


def lane_sum(h):
    out = h[:, :128]
    for g in range(1, h.shape[1] // 128):
        out = out + h[:, g * 128:(g + 1) * 128]
    return out


DEVICES = 8
CHIPS = 4
EXTRA = 8
CHUNK = 512
AHEAD = 4
UPDATE_AT = 5
RELAY_AT = 0


def main_kernel(sweeps, grid_cols, counts, w_in, h_in,
                c_par, h_pair, h_last, w_out,
                h_ref, wb_ref, ws_ref, hs_acc, wsl_ref, wfin, cbuf, hbuf, nh_ref, wbt_ref, wb0, wbt0, ws0_buf, ws0_ref, hs_first, acc, nw_recv, ws_buf, ws_half, hs_row,
                csem, psem, hsem, hhsem, c_send, c_got, w0_send, w0_got,
                nw_send, nw_got, wb_send, wb_got, ws_send, ws_got,
                mate_recv, mate_send, mate_got, h_send, h_got, out_sem, wf_send, wf_got, fin_send, fin_got):
    row, col = lax.axis_index("row"), lax.axis_index("col")
    me = row * grid_cols + col
    docs, full = counts.shape
    topics, width = h_ref.shape
    blocks = width // BV
    chunks = width // CHUNK
    part = docs // DEVICES
    partner = {"row": 1 - row, "col": col}
    mesh_id = pl.DeviceIdType.MESH

    def remote(src, dst, send, got, where):
        return pltpu.make_async_remote_copy(src, dst, send, got, device_id=where, device_id_type=mesh_id)

    def peer(p):
        other = lax.rem(me + p, DEVICES)
        return {"row": other // grid_cols, "col": lax.rem(other, grid_cols)}, other

    core, chip = lax.rem(col, 2), me // 2
    mate = {"row": row, "col": col + 1 - 2 * core}

    def mate_copy(half):
        return remote(acc.at[half, 1 - core], mate_recv.at[half], mate_send.at[half], mate_got.at[half], mate)

    def nw_copy(p, half):
        there = lax.rem(chip + p, CHIPS)
        d = 2 * there + core
        return remote(acc.at[half, core, there], nw_recv.at[half, p], nw_send.at[half, p], nw_got.at[half, p],
                      {"row": d // grid_cols, "col": lax.rem(d, grid_cols)})

    def wb_copy(p, half):
        mine = wb_ref.at[half, pl.ds(pl.multiple_of(me * part, part), part)]
        return remote(mine, mine, wb_send.at[half, p], wb_got.at[half, p], peer(p)[0])

    def ws_copy(p, half):
        return remote(ws_buf.at[half, 0], ws_buf.at[half, p], ws_send.at[half, p], ws_got.at[half, p], peer(p)[0])

    def row_peer(q):
        there = lax.rem(col + q, grid_cols)
        return {"row": row, "col": there}, there

    def first_copy(q):
        where, there = row_peer(q)
        return remote(acc.at[row, :, there], nw_recv.at[row, pl.ds(2 * q, 2)], fin_send.at[q], fin_got.at[q], where)

    def first_wb(half, q):
        where = row_peer(q)[0] if q else partner
        mine = wb_ref.at[half, pl.ds(pl.multiple_of(col * 2 * part, 2 * part), 2 * part)]
        return remote(mine, mine, wb_send.at[half, q], wb_got.at[half, q], where)

    def first_ws(half, q):
        where = row_peer(q)[0] if q else partner
        return remote(ws_buf.at[half, 0], ws_buf.at[half, q], ws_send.at[half, q], ws_got.at[half, q], where)

    def first_owner(b):
        d = 2 * col + b
        return remote(wfin.at[b], wsl_ref.at[row], wf_send.at[b], wf_got.at[row],
                      {"row": d // grid_cols, "col": lax.rem(d, grid_cols)})

    def chunk_copy(j):
        theirs = pl.ds(pl.multiple_of((1 - row) * width + j * CHUNK, CHUNK), CHUNK)
        here = pl.ds(pl.multiple_of(j * CHUNK, CHUNK), CHUNK)
        return remote(counts.at[:, theirs], c_par.at[:, here], c_send.at[j], c_got.at[j], partner)

    half_docs = docs // 2

    def w0_part(of_core):
        return pl.ds(pl.multiple_of(of_core * half_docs, half_docs), half_docs)

    def w0_copies():
        at = w0_part(core)
        return [
            remote(wb0.at[0, at], wb0.at[1, at], w0_send.at[0], w0_got.at[0], partner),
            remote(ws0_buf.at[0], ws0_buf.at[1], w0_send.at[1], w0_got.at[1], partner),
        ]

    def w0_forward():
        at = w0_part(core)
        return remote(wb0.at[1, at], wb0.at[1, at], w0_send.at[2], w0_got.at[2], mate)

    def local(src, dst, sem):
        return pltpu.make_async_copy(src, dst, sem)

    def c_start(half, j, slot):
        @pl.when(row == half)
        def _():
            local(counts.at[:, pl.ds(pl.multiple_of(row * width + j * BV, BV), BV)], cbuf.at[slot], csem.at[slot]).start()

        @pl.when(row != half)
        def _():
            local(c_par.at[:, pl.ds(pl.multiple_of(j * BV, BV), BV)], cbuf.at[slot], csem.at[slot]).start()

    def c_wait(slot):
        local(counts.at[:, pl.ds(0, BV)], cbuf.at[slot], csem.at[slot]).wait()

    def first_c(i, slot):
        block = lax.rem(row * blocks + i, 2 * blocks)
        return local(counts.at[:, pl.ds(pl.multiple_of(block * BV, BV), BV)], cbuf.at[slot], csem.at[slot])

    def first_h(j, slot):
        at = pl.ds(pl.multiple_of((1 - row) * width + j * BV, BV), BV)
        return local(h_in.at[:, at], hbuf.at[slot], hsem.at[slot])

    def own_chunk(j, slot):
        at = pl.ds(pl.multiple_of(row * width + j * CHUNK, CHUNK), CHUNK)
        return local(counts.at[:, at], cbuf.at[slot, :, pl.ds(0, CHUNK)], csem.at[slot])

    def par_chunk(j, slot):
        at = pl.ds(pl.multiple_of(j * CHUNK, CHUNK), CHUNK)
        return local(c_par.at[:, at], cbuf.at[slot, :, pl.ds(CHUNK, CHUNK)], psem.at[slot])

    def acc_add(half, res):
        for b in range(DEVICES):
            acc[half, b % 2, b // 2, pl.ds(0, part)] += res[b * part:(b + 1) * part]

    def acc_sums(half):
        for b in range(DEVICES):
            acc[half, b % 2, b // 2, pl.ds(part, EXTRA)] = hs_row[...]

    def acc_zero(half):
        acc[half] = jnp.zeros(acc.shape[1:], F32)

    def send_nw(half):
        acc_sums(half)
        mate_copy(half).start()

    def relay(half):
        mate_copy(half).wait_recv()
        acc[half, core] += mate_recv[half]
        for p in range(1, CHIPS):
            nw_copy(p, half).start()

    def publish(half, total):
        new = wsl_ref[half] * total[:part] / total[part:part + 1]
        wsl_ref[half] = new
        wb_ref[half, pl.ds(pl.multiple_of(me * part, part), part)] = new.astype(BF16)
        ws_buf[half, 0] = jnp.broadcast_to(jnp.sum(new, axis=0, keepdims=True), (EXTRA, topics))
        for p in range(1, DEVICES):
            wb_copy(p, half).start()
            ws_copy(p, half).start()

    def sent_w(half):
        for p in range(1, DEVICES):
            wb_copy(p, half).wait_send()
            ws_copy(p, half).wait_send()

    def sent_nw(half):
        mate_copy(half).wait_send()
        for p in range(1, CHIPS):
            nw_copy(p, half).wait_send()

    def owner_update(half):
        for p in range(1, CHIPS):
            nw_copy(p, half).wait_recv()
        total = acc[half, core, chip]
        for p in range(1, CHIPS):
            total = total + nw_recv[half, p]
        publish(half, total)

    def receive_w(half):
        for p in range(1, DEVICES):
            wb_copy(p, half).wait_recv()
            ws_copy(p, half).wait_recv()
        wbt_ref[half] = wb_ref[half].T
        total = ws_buf[half, 0]
        for p in range(1, DEVICES):
            total = total + ws_buf[half, p]
        return total

    def wfin_copy(half):
        return remote(wsl_ref.at[half], wfin.at[lax.rem(me, 2)], wf_send.at[half], wf_got.at[lax.rem(me, 2)],
                      {"row": jnp.int32(half), "col": me // 2})

    def wfin_here(half):
        return jnp.logical_and(row == half, col == me // 2)

    def fin_copy(q):
        there = lax.rem(col + q, grid_cols)
        return remote(acc.at[:, :, there], nw_recv.at[:, pl.ds(2 * q, 2)], fin_send.at[q], fin_got.at[q],
                      {"row": row, "col": there})

    def fin_cross():
        pair = nw_recv.at[1 - row, pl.ds(0, 2)]
        return remote(pair, pair, fin_send.at[0], fin_got.at[0], partner)

    def out_copy(q):
        mine = w_out.at[pl.ds(pl.multiple_of(col * 2 * part, 2 * part), 2 * part)]
        return remote(mine, mine, fin_send.at[grid_cols + q], fin_got.at[grid_cols + q],
                      {"row": row, "col": lax.rem(col + q, grid_cols)})

    def h_remote(j):
        at = pl.ds(pl.multiple_of(j * CHUNK, CHUNK), CHUNK)
        return remote(h_ref.at[:, at], h_pair.at[row, :, at], h_send.at[j], h_got.at[j], partner)

    def h_local(j):
        at = pl.ds(pl.multiple_of(j * CHUNK, CHUNK), CHUNK)
        return local(h_ref.at[:, at], h_pair.at[row, :, at], out_sem.at[j])

    def to_row(lanes):
        return jnp.broadcast_to(jnp.sum(lanes.T, axis=0, keepdims=True), (EXTRA, topics))

    def to_lanes(sums):
        return jnp.broadcast_to(sums[:1], (128, topics)).T

    barrier = pltpu.get_barrier_semaphore()
    for p in range(1, DEVICES):
        pl.semaphore_signal(barrier, inc=1, device_id=peer(p)[0], device_id_type=mesh_id)

    own_h = local(h_in.at[:, pl.ds(pl.multiple_of(row * width, width), width)], h_ref, hhsem)
    own_h.start()
    first_c(0, 0).start()
    wb0[0] = w_in[...].astype(BF16)
    ws0_buf[0] = jnp.broadcast_to(jnp.sum(w_in[...], axis=0, keepdims=True), (EXTRA, topics))
    pl.semaphore_wait(barrier, DEVICES - 1)
    for copy in w0_copies():
        copy.start()
    for j in range(AHEAD):
        chunk_copy(j).start()
    wbt0[0] = wb0[0].T
    acc_zero(0)
    acc_zero(1)
    hs_first[...] = jnp.zeros_like(hs_first)
    hs_acc[...] = jnp.zeros_like(hs_acc)
    own_h.wait()

    def first_own(j, carry):
        slot = lax.rem(j, 2)
        first_c(j, slot).wait()
        first_c(j + 1, 1 - slot).start()

        @pl.when(j == blocks - 1)
        def _():
            first_h(0, 0).start()

        at = pl.ds(pl.multiple_of(j * BV, BV), BV)
        h = h_ref[:, at]
        hb = h.astype(BF16)
        q = ratio(cbuf[slot], dot(wb0[0], hb))
        acc_add(row, dot_t(q, hb))
        nh_ref[:, at] = dot(wbt0[0], q)
        hs_first[...] += lane_sum(h)
        return carry

    lax.fori_loop(0, blocks, first_own, 0)

    def first_other(j, carry):
        slot = lax.rem(j, 2)
        first_c(blocks + j, slot).wait()
        first_h(j, slot).wait()

        @pl.when(j < blocks - 1)
        def _():
            first_c(blocks + j + 1, 1 - slot).start()
            first_h(j + 1, 1 - slot).start()

        h = hbuf[slot]
        hb = h.astype(BF16)
        q = ratio(cbuf[slot], dot(wb0[0], hb))
        acc_add(row, dot_t(q, hb))
        hs_first[...] += lane_sum(h)
        return carry

    lax.fori_loop(0, blocks, first_other, 0)

    hs_row[...] = to_row(hs_first[...])
    acc_sums(row)
    for q in range(1, grid_cols):
        first_copy(q).start()
    own_chunk(0, 0).start()
    for copy in w0_copies():
        copy.wait_recv()
    w0_forward().start()
    for q in range(1, grid_cols):
        first_copy(q).wait_recv()
    total = acc[row, :, col]
    for q in range(1, grid_cols):
        total = total + nw_recv[row, pl.ds(2 * q, 2)]
    sums = jnp.zeros((1, topics), F32)
    for b in range(2):
        at = pl.ds(pl.multiple_of((2 * col + b) * part, part), part)
        new = w_in[at] * total[b, :part] / total[b, part:part + 1]
        wfin[b] = new
        wb_ref[row, at] = new.astype(BF16)
        sums = sums + jnp.sum(new, axis=0, keepdims=True)
    ws_buf[row, 0] = jnp.broadcast_to(sums, (EXTRA, topics))
    for q in range(grid_cols):
        first_wb(row, q).start()
        first_ws(row, q).start()
    for b in range(2):
        @pl.when(2 * col + b == me)
        def _():
            wsl_ref[row] = wfin[b]

        @pl.when(2 * col + b != me)
        def _():
            first_owner(b).start()

    first_wb(1 - row, 0).wait_recv()
    first_ws(1 - row, 0).wait_recv()
    for q in range(1, grid_cols):
        first_wb(1 - row, q).start()
        first_ws(1 - row, q).start()
    w0_forward().wait_recv()
    wbt0[1] = wb0[1].T
    ws0_ref[...] = to_lanes(ws0_buf[0] + ws0_buf[1])
    hs_first[...] = jnp.zeros_like(hs_first)
    for q in range(1, grid_cols):
        first_copy(q).wait_send()
    acc_zero(row)
    total = ws_buf[0, 0] + ws_buf[1, 0]
    for half in range(2):
        for q in range(1, grid_cols):
            first_wb(half, q).wait_recv()
            first_ws(half, q).wait_recv()
            total = total + ws_buf[half, q]
        wbt_ref[half] = wb_ref[half].T
    ws_ref[...] = to_lanes(total)

    def both_halves(slot, h):
        hb = h.astype(BF16)
        q = ratio(cbuf[slot, :, pl.ds(0, CHUNK)], dot(wb_ref[row], hb))
        acc_add(row, dot_t(q, hb))
        nh = dot(wbt_ref[row], q)
        q = ratio(cbuf[slot, :, pl.ds(CHUNK, CHUNK)], dot(wb_ref[1 - row], hb))
        acc_add(1 - row, dot_t(q, hb))
        nh = nh + dot(wbt_ref[1 - row], q)
        return h * nh / ws_ref[:, :1]

    def chunk_step(j, carry):
        slot = lax.rem(j, 2)
        chunk_copy(j).wait_recv()
        par_chunk(j, slot).start()
        chunk_copy(j).wait_send()

        @pl.when(j < chunks // 2)
        def _():
            chunk_copy(j + AHEAD).start()

        @pl.when(jnp.logical_and(j >= chunks // 2 + AHEAD - 2, j < chunks - 2))
        def _():
            chunk_copy(j + 2).start()

        own_chunk(j, slot).wait()

        @pl.when(j < chunks - 1)
        def _():
            own_chunk(j + 1, 1 - slot).start()

        at = pl.ds(pl.multiple_of(j * CHUNK, CHUNK), CHUNK)
        h = h_ref[:, at]
        par_chunk(j, slot).wait()
        other = cbuf[slot, :, pl.ds(CHUNK, CHUNK)]
        q = ratio(other, dot(wb0[1], h.astype(BF16)))
        h = h * (nh_ref[:, at] + dot(wbt0[1], q)) / ws0_ref[:, :1]
        hs_first[...] += lane_sum(h)
        h = both_halves(slot, h)
        h_ref[:, at] = h
        hs_acc[...] += lane_sum(h)
        return carry

    lax.fori_loop(0, chunks, chunk_step, 0)
    for copy in w0_copies():
        copy.wait_send()
    w0_forward().wait_send()
    first_wb(row, 0).wait_send()
    first_ws(row, 0).wait_send()
    for half in range(2):
        for q in range(1, grid_cols):
            first_wb(half, q).wait_send()
            first_ws(half, q).wait_send()

        @pl.when(2 * col + half != me)
        def _():
            first_owner(half).wait_send()

        @pl.when(jnp.logical_not(wfin_here(half)))
        def _():
            remote(wfin.at[0], wsl_ref.at[half], wf_send.at[0], wf_got.at[half], partner).wait_recv()

    hs_row[...] = to_row(hs_first[...])
    send_nw(0)
    send_nw(1)
    c_start(0, 0, 0)
    relay(0)
    owner_update(0)

    def step(half, j, last):
        slot = lax.rem(j, 2)
        c_wait(slot)

        @pl.when(j < blocks - 1)
        def _():
            c_start(half, j + 1, 1 - slot)

        @pl.when(jnp.logical_and(j == blocks - 1, jnp.logical_not(last)))
        def _():
            c_start(1 - half, 0, 1 - slot)

        at = pl.ds(pl.multiple_of(j * BV, BV), BV)
        hb = h_ref[:, at].astype(BF16)
        q = ratio(cbuf[slot], dot(wb_ref[half], hb))
        acc_add(half, dot_t(q, hb))
        nh = dot(wbt_ref[half], q)
        if half == 0:
            nh_ref[:, at] = nh
        else:
            new = h_ref[:, at] * (nh_ref[:, at] + nh) / ws_ref[:, :1]
            h_ref[:, at] = new
            hs_acc[...] += lane_sum(new)

    def one_sweep(s, carry):
        last = s == sweeps - 1
        ws_half[...] = receive_w(0)
        sent_w(0)
        hs_row[...] = to_row(hs_acc[...])
        hs_acc[...] = jnp.zeros_like(hs_acc)
        sent_nw(0)
        acc_zero(0)

        def step_a(j, carry):
            @pl.when(j == RELAY_AT)
            def _():
                relay(1)

            @pl.when(j == UPDATE_AT)
            def _():
                owner_update(1)

            step(0, j, False)
            return carry

        lax.fori_loop(0, blocks, step_a, 0)
        send_nw(0)
        ws_ref[...] = to_lanes(ws_half[...] + receive_w(1))
        sent_w(1)
        sent_nw(1)
        acc_zero(1)

        def step_b(j, carry):
            @pl.when(j == RELAY_AT)
            def _():
                relay(0)

            @pl.when(j == UPDATE_AT)
            def _():
                owner_update(0)

            step(1, j, last)
            return carry

        lax.fori_loop(0, blocks, step_b, 0)
        send_nw(1)
        return carry

    lax.fori_loop(0, sweeps, one_sweep, 0)
    own_chunk(0, 0).start()
    par_chunk(0, 0).start()
    relay(1)
    owner_update(1)
    for half in range(2):
        @pl.when(wfin_here(half))
        def _():
            wfin[lax.rem(me, 2)] = wsl_ref[half]

        @pl.when(jnp.logical_not(wfin_here(half)))
        def _():
            wfin_copy(half).start()

    hs_row[...] = to_row(hs_acc[...])
    for half in range(2):
        sent_nw(half)
        acc_zero(half)
    ws_ref[...] = to_lanes(receive_w(0) + receive_w(1))

    def last_step(j, carry):
        slot = lax.rem(j, 2)
        own_chunk(j, slot).wait()
        par_chunk(j, slot).wait()

        @pl.when(j < chunks - 1)
        def _():
            own_chunk(j + 1, 1 - slot).start()
            par_chunk(j + 1, 1 - slot).start()

        @pl.when(j > 0)
        def _():
            h_remote(j - 1).start()
            h_local(j - 1).start()

        at = pl.ds(pl.multiple_of(j * CHUNK, CHUNK), CHUNK)
        h_ref[:, at] = both_halves(slot, h_ref[:, at])
        return carry

    lax.fori_loop(0, chunks, last_step, 0)
    for half in range(2):
        acc_sums(half)
    h_local(chunks - 1).start()
    tail = local(h_ref.at[:, pl.ds(width - CHUNK, CHUNK)], h_last, hhsem)
    tail.start()
    for q in range(1, grid_cols):
        fin_copy(q).start()
    for half in range(2):
        @pl.when(jnp.logical_not(wfin_here(half)))
        def _():
            wfin_copy(half).wait_send()

    for parity in range(2):
        @pl.when(2 * col + parity != me)
        def _():
            remote(wsl_ref.at[0], wfin.at[parity], wf_send.at[0], wf_got.at[parity], partner).wait_recv()

    for q in range(1, grid_cols):
        fin_copy(q).wait_recv()
    ours = acc[row, :, col]
    theirs = acc[1 - row, :, col]
    for q in range(1, grid_cols):
        ours = ours + nw_recv[row, pl.ds(2 * q, 2)]
        theirs = theirs + nw_recv[1 - row, pl.ds(2 * q, 2)]
    nw_recv[1 - row, pl.ds(0, 2)] = theirs
    fin_cross().start()
    fin_cross().wait_recv()
    total = ours + nw_recv[row, pl.ds(0, 2)]
    new = wfin[...] * total[:, :part] / total[:1, part:part + 1]
    for b in range(2):
        w_out[pl.ds(pl.multiple_of((2 * col + b) * part, part), part)] = new[b]
    for q in range(1, grid_cols):
        out_copy(q).start()
    for half in range(2):
        sent_w(half)
    for q in range(1, grid_cols):
        out_copy(q).wait()
        fin_copy(q).wait_send()
    fin_cross().wait_send()

    tail.wait()

    def drain(j, carry):
        h_remote(j).wait_recv()
        h_remote(j).wait_send()
        h_local(j).wait()
        return carry

    lax.fori_loop(0, chunks - 1, drain, 0)
    h_local(chunks - 1).wait()


PLACE = 2048


def place_kernel(h_pair, h_out, buf, in_sem, out_sem):
    row = lax.axis_index("row")
    width = h_pair.shape[2]
    jobs = []
    for other in range(2):
        half = 1 - row if other else row
        for start in range(0, width, PLACE):
            size = PLACE - CHUNK if other and start + PLACE == width else PLACE
            n = len(jobs)
            held = buf.at[n, :, pl.ds(0, size)]
            jobs.append((
                pltpu.make_async_copy(h_pair.at[half, :, pl.ds(start, size)], held, in_sem.at[n]),
                pltpu.make_async_copy(held, h_out.at[:, pl.ds(pl.multiple_of(half * width + start, PLACE), size)], out_sem.at[n]),
            ))
    for load, _ in jobs:
        load.start()
    for load, store in jobs:
        load.wait()
        store.start()
    for _, store in jobs:
        store.wait()


def cost(docs, columns, topics, dots):
    return pl.CostEstimate(flops=int(2 * docs * columns * topics * dots), bytes_accessed=2 * docs * columns, transcendentals=0)


def solution(mesh):
    rows, cols = mesh.shape["row"], mesh.shape["col"]

    def body(counts, w_own, h_blk):
        docs, width = counts.shape
        topics = w_own.shape[1]
        mine = width // rows
        sds = jax.ShapeDtypeStruct
        lanes = (topics, 128)
        part = docs // DEVICES
        vmem, hbm = pl.BlockSpec(memory_space=pltpu.VMEM), pl.BlockSpec(memory_space=pl.ANY)
        dma = pltpu.SemaphoreType.DMA
        V = pltpu.VMEM
        exchange = V((rows, DEVICES, part + EXTRA, topics), F32)
        partial = V((rows, 2, CHIPS, part + EXTRA, topics), F32)
        pieces = mine // CHUNK
        c_par, h_pair, h_last, w_out = pl.pallas_call(
            functools.partial(main_kernel, SWEEPS - 3, cols),
            in_specs=[hbm, vmem, hbm],
            out_specs=[hbm, hbm, hbm, vmem],
            out_shape=[sds((docs, mine), BF16), sds((rows, topics, mine), F32), sds((topics, CHUNK), F32),
                       sds((docs, topics), F32)],
            scratch_shapes=[
                V((topics, mine), F32), V((rows, docs, topics), BF16), V(lanes, F32), V(lanes, F32),
                V((rows, part, topics), F32), V((2, part, topics), F32),
                V((2, docs, BV), BF16), V((2, topics, BV), F32), V((topics, mine), F32), V((rows, topics, docs), BF16),
                V((2, docs, topics), BF16), V((2, topics, docs), BF16), V((2, EXTRA, topics), F32), V(lanes, F32),
                V(lanes, F32), partial, exchange, V((rows, DEVICES, EXTRA, topics), F32),
                V((EXTRA, topics), F32), V((EXTRA, topics), F32),
                dma((2,)), dma((2,)), dma((2,)), dma, dma((pieces,)), dma((pieces,)), dma((3,)), dma((3,)),
            ] + [dma((rows, DEVICES))] * 6 + [V((rows, CHIPS, part + EXTRA, topics), F32), dma((rows,)), dma((rows,))] + [dma((pieces,))] * 3 + [dma((2,))] * 2 + [dma((2 * cols,))] * 2,
            compiler_params=pltpu.CompilerParams(vmem_limit_bytes=VMEM, collective_id=0, has_side_effects=True),
            cost_estimate=cost(rows * docs, mine, topics, 18), name="main",
        )(counts, w_own, h_blk)
        other = lax.ppermute(h_last, "row", [(0, 1), (1, 0)])
        row = lax.axis_index("row")
        jobs = 2 * mine // PLACE
        h_out = pl.pallas_call(
            place_kernel,
            in_specs=[hbm], out_specs=hbm, out_shape=sds((topics, width), F32),
            scratch_shapes=[V((jobs, topics, PLACE), F32), dma((jobs,)), dma((jobs,))],
            compiler_params=pltpu.CompilerParams(vmem_limit_bytes=VMEM),
            cost_estimate=pl.CostEstimate(flops=10 ** 8, bytes_accessed=8 * topics * width, transcendentals=0), name="place",
        )(h_pair)
        h_out = lax.dynamic_update_slice(h_out, other, (0, (1 - row) * mine + mine - CHUNK))
        return w_out, h_out

    return jax.shard_map(
        body,
        mesh=mesh,
        in_specs=(P(("part", "row"), "col"), P(("part", "row"), None), P("part", "col")),
        out_specs=(P(("part", "row"), None), P("part", "col")),
        check_vma=False,
    )
```

```python
import functools

import jax
import jax.numpy as jnp
from jax import lax
from jax.experimental import pallas as pl
from jax.experimental.pallas import tpu as pltpu
from jax.sharding import PartitionSpec as P

SWEEPS = 6
F32 = jnp.float32
BF16 = jnp.bfloat16
BV = 1024
VMEM = 60 * 1024 * 1024


def dot(a, b):
    return jnp.dot(a, b, preferred_element_type=F32)


def dot_t(a, b):
    return lax.dot_general(a, b, (((1,), (1,)), ((), ())), preferred_element_type=F32)


def ratio(c, z):
    return (c.astype(F32) / z).astype(BF16)


def lane_sum(h):
    out = h[:, :128]
    for g in range(1, h.shape[1] // 128):
        out = out + h[:, g * 128:(g + 1) * 128]
    return out


DEVICES = 8
CHIPS = 4
EXTRA = 8
CHUNK = 512
ARRIVE = 256
AHEAD = 8
UPDATE_AT = 5
RELAY_AT = 0


def main_kernel(sweeps, grid_cols, counts, w_in, h_in,
                c_par, h_pair, h_last, w_out,
                h_ref, wb_ref, ws_ref, hs_acc, wsl_ref, wfin, cbuf, hbuf, nh_ref, wbt_ref, wb0, wbt0, ws0_buf, ws0_ref, hs_first, acc, nw_recv, ws_buf, ws_half, hs_row,
                csem, psem, hsem, hhsem, c_send, c_got, w0_send, w0_got,
                nw_send, nw_got, wb_send, wb_got, ws_send, ws_got,
                mate_recv, mate_send, mate_got, h_send, h_got, out_sem, wf_send, wf_got, fin_send, fin_got):
    row, col = lax.axis_index("row"), lax.axis_index("col")
    me = row * grid_cols + col
    docs, full = counts.shape
    topics, width = h_ref.shape
    blocks = width // BV
    chunks = width // CHUNK
    arrivals = width // ARRIVE
    part = docs // DEVICES
    partner = {"row": 1 - row, "col": col}
    mesh_id = pl.DeviceIdType.MESH

    def remote(src, dst, send, got, where):
        return pltpu.make_async_remote_copy(src, dst, send, got, device_id=where, device_id_type=mesh_id)

    def peer(p):
        other = lax.rem(me + p, DEVICES)
        return {"row": other // grid_cols, "col": lax.rem(other, grid_cols)}, other

    core, chip = lax.rem(col, 2), me // 2
    mate = {"row": row, "col": col + 1 - 2 * core}

    def mate_copy(half):
        return remote(acc.at[half, 1 - core], mate_recv.at[half], mate_send.at[half], mate_got.at[half], mate)

    def nw_copy(p, half):
        there = lax.rem(chip + p, CHIPS)
        d = 2 * there + core
        return remote(acc.at[half, core, there], nw_recv.at[half, p], nw_send.at[half, p], nw_got.at[half, p],
                      {"row": d // grid_cols, "col": lax.rem(d, grid_cols)})

    def wb_copy(p, half):
        mine = wb_ref.at[half, pl.ds(pl.multiple_of(me * part, part), part)]
        return remote(mine, mine, wb_send.at[half, p], wb_got.at[half, p], peer(p)[0])

    def ws_copy(p, half):
        return remote(ws_buf.at[half, 0], ws_buf.at[half, p], ws_send.at[half, p], ws_got.at[half, p], peer(p)[0])

    def row_peer(q):
        there = lax.rem(col + q, grid_cols)
        return {"row": row, "col": there}, there

    def first_copy(q):
        where, there = row_peer(q)
        return remote(acc.at[row, :, there], nw_recv.at[row, pl.ds(2 * q, 2)], fin_send.at[q], fin_got.at[q], where)

    def first_wb(half, q):
        where = row_peer(q)[0] if q else partner
        mine = wb_ref.at[half, pl.ds(pl.multiple_of(col * 2 * part, 2 * part), 2 * part)]
        return remote(mine, mine, wb_send.at[half, q], wb_got.at[half, q], where)

    def first_ws(half, q):
        where = row_peer(q)[0] if q else partner
        return remote(ws_buf.at[half, 0], ws_buf.at[half, q], ws_send.at[half, q], ws_got.at[half, q], where)

    def first_owner(b):
        d = 2 * col + b
        return remote(wfin.at[b], wsl_ref.at[row], wf_send.at[b], wf_got.at[row],
                      {"row": d // grid_cols, "col": lax.rem(d, grid_cols)})

    def chunk_copy(j):
        theirs = pl.ds(pl.multiple_of((1 - row) * width + j * ARRIVE, ARRIVE), ARRIVE)
        here = pl.ds(pl.multiple_of(j * ARRIVE, ARRIVE), ARRIVE)
        return remote(counts.at[:, theirs], c_par.at[:, here], c_send.at[j], c_got.at[j], partner)

    def w0_copies():
        at = pl.ds(pl.multiple_of(col * 2 * part, 2 * part), 2 * part)
        return [
            remote(wb0.at[0, at], wb0.at[1, at], w0_send.at[0], w0_got.at[0], partner),
            remote(ws0_buf.at[0], ws0_buf.at[1], w0_send.at[grid_cols], w0_got.at[grid_cols], partner),
        ]

    def w0_forward(q):
        at = pl.ds(pl.multiple_of(col * 2 * part, 2 * part), 2 * part)
        return remote(wb0.at[1, at], wb0.at[1, at], w0_send.at[q], w0_got.at[q], row_peer(q)[0])

    def local(src, dst, sem):
        return pltpu.make_async_copy(src, dst, sem)

    def c_start(half, j, slot):
        @pl.when(row == half)
        def _():
            local(counts.at[:, pl.ds(pl.multiple_of(row * width + j * BV, BV), BV)], cbuf.at[slot], csem.at[slot]).start()

        @pl.when(row != half)
        def _():
            local(c_par.at[:, pl.ds(pl.multiple_of(j * BV, BV), BV)], cbuf.at[slot], csem.at[slot]).start()

    def c_wait(slot):
        local(counts.at[:, pl.ds(0, BV)], cbuf.at[slot], csem.at[slot]).wait()

    def first_c(i, slot):
        block = lax.rem(row * blocks + i, 2 * blocks)
        return local(counts.at[:, pl.ds(pl.multiple_of(block * BV, BV), BV)], cbuf.at[slot], csem.at[slot])

    def first_h(j, slot):
        at = pl.ds(pl.multiple_of((1 - row) * width + j * BV, BV), BV)
        return local(h_in.at[:, at], hbuf.at[slot], hsem.at[slot])

    def own_chunk(j, slot, size=CHUNK):
        at = pl.ds(pl.multiple_of(row * width + j * size, size), size)
        return local(counts.at[:, at], cbuf.at[slot, :, pl.ds(0, size)], csem.at[slot])

    def par_chunk(j, slot, size=CHUNK):
        at = pl.ds(pl.multiple_of(j * size, size), size)
        return local(c_par.at[:, at], cbuf.at[slot, :, pl.ds(CHUNK, size)], psem.at[slot])

    def acc_add(half, res):
        for b in range(DEVICES):
            acc[half, b % 2, b // 2, pl.ds(0, part)] += res[b * part:(b + 1) * part]

    def acc_sums(half):
        for b in range(DEVICES):
            acc[half, b % 2, b // 2, pl.ds(part, EXTRA)] = hs_row[...]

    def acc_zero(half):
        acc[half] = jnp.zeros(acc.shape[1:], F32)

    def send_nw(half):
        acc_sums(half)
        mate_copy(half).start()

    def relay(half):
        mate_copy(half).wait_recv()
        acc[half, core] += mate_recv[half]
        for p in range(1, CHIPS):
            nw_copy(p, half).start()

    def publish(half, total):
        new = wsl_ref[half] * total[:part] / total[part:part + 1]
        wsl_ref[half] = new
        wb_ref[half, pl.ds(pl.multiple_of(me * part, part), part)] = new.astype(BF16)
        ws_buf[half, 0] = jnp.broadcast_to(jnp.sum(new, axis=0, keepdims=True), (EXTRA, topics))
        for p in range(1, DEVICES):
            wb_copy(p, half).start()
            ws_copy(p, half).start()

    def sent_w(half):
        for p in range(1, DEVICES):
            wb_copy(p, half).wait_send()
            ws_copy(p, half).wait_send()

    def sent_nw(half):
        mate_copy(half).wait_send()
        for p in range(1, CHIPS):
            nw_copy(p, half).wait_send()

    def owner_update(half):
        for p in range(1, CHIPS):
            nw_copy(p, half).wait_recv()
        total = acc[half, core, chip]
        for p in range(1, CHIPS):
            total = total + nw_recv[half, p]
        publish(half, total)

    def receive_w(half):
        for p in range(1, DEVICES):
            wb_copy(p, half).wait_recv()
            ws_copy(p, half).wait_recv()
        wbt_ref[half] = wb_ref[half].T
        total = ws_buf[half, 0]
        for p in range(1, DEVICES):
            total = total + ws_buf[half, p]
        return total

    def wfin_copy(half):
        return remote(wsl_ref.at[half], wfin.at[lax.rem(me, 2)], wf_send.at[half], wf_got.at[lax.rem(me, 2)],
                      {"row": jnp.int32(half), "col": me // 2})

    def wfin_here(half):
        return jnp.logical_and(row == half, col == me // 2)

    def fin_copy(q):
        there = lax.rem(col + q, grid_cols)
        return remote(acc.at[:, :, there], nw_recv.at[:, pl.ds(2 * q, 2)], fin_send.at[q], fin_got.at[q],
                      {"row": row, "col": there})

    def fin_cross():
        pair = nw_recv.at[1 - row, pl.ds(0, 2)]
        return remote(pair, pair, fin_send.at[0], fin_got.at[0], partner)

    def out_copy(q):
        mine = w_out.at[pl.ds(pl.multiple_of(col * 2 * part, 2 * part), 2 * part)]
        return remote(mine, mine, fin_send.at[grid_cols + q], fin_got.at[grid_cols + q],
                      {"row": row, "col": lax.rem(col + q, grid_cols)})

    def h_remote(j):
        at = pl.ds(pl.multiple_of(j * CHUNK, CHUNK), CHUNK)
        return remote(h_ref.at[:, at], h_pair.at[row, :, at], h_send.at[j], h_got.at[j], partner)

    def h_local(j):
        at = pl.ds(pl.multiple_of(j * CHUNK, CHUNK), CHUNK)
        return local(h_ref.at[:, at], h_pair.at[row, :, at], out_sem.at[j])

    def to_row(lanes):
        return jnp.broadcast_to(jnp.sum(lanes.T, axis=0, keepdims=True), (EXTRA, topics))

    def to_lanes(sums):
        return jnp.broadcast_to(sums[:1], (128, topics)).T

    barrier = pltpu.get_barrier_semaphore()
    for p in range(1, DEVICES):
        pl.semaphore_signal(barrier, inc=1, device_id=peer(p)[0], device_id_type=mesh_id)

    own_h = local(h_in.at[:, pl.ds(pl.multiple_of(row * width, width), width)], h_ref, hhsem)
    own_h.start()
    first_c(0, 0).start()
    wb0[0] = w_in[...].astype(BF16)
    ws0_buf[0] = jnp.broadcast_to(jnp.sum(w_in[...], axis=0, keepdims=True), (EXTRA, topics))
    pl.semaphore_wait(barrier, DEVICES - 1)
    for copy in w0_copies():
        copy.start()
    for j in range(AHEAD):
        chunk_copy(j).start()
    wbt0[0] = wb0[0].T
    acc_zero(0)
    acc_zero(1)
    hs_first[...] = jnp.zeros_like(hs_first)
    hs_acc[...] = jnp.zeros_like(hs_acc)
    own_h.wait()

    def first_own(j, carry):
        slot = lax.rem(j, 2)
        first_c(j, slot).wait()
        first_c(j + 1, 1 - slot).start()

        @pl.when(j == blocks - 1)
        def _():
            first_h(0, 0).start()

        at = pl.ds(pl.multiple_of(j * BV, BV), BV)
        h = h_ref[:, at]
        hb = h.astype(BF16)
        q = ratio(cbuf[slot], dot(wb0[0], hb))
        acc_add(row, dot_t(q, hb))
        nh_ref[:, at] = dot(wbt0[0], q)
        hs_first[...] += lane_sum(h)
        return carry

    lax.fori_loop(0, blocks, first_own, 0)

    def first_other(j, carry):
        slot = lax.rem(j, 2)
        first_c(blocks + j, slot).wait()
        first_h(j, slot).wait()

        @pl.when(j < blocks - 1)
        def _():
            first_c(blocks + j + 1, 1 - slot).start()
            first_h(j + 1, 1 - slot).start()

        h = hbuf[slot]
        hb = h.astype(BF16)
        q = ratio(cbuf[slot], dot(wb0[0], hb))
        acc_add(row, dot_t(q, hb))
        hs_first[...] += lane_sum(h)
        return carry

    lax.fori_loop(0, blocks, first_other, 0)

    hs_row[...] = to_row(hs_first[...])
    acc_sums(row)
    for q in range(1, grid_cols):
        first_copy(q).start()
    own_chunk(0, 0, ARRIVE).start()
    for copy in w0_copies():
        copy.wait_recv()
    for q in range(1, grid_cols):
        w0_forward(q).start()
    for q in range(1, grid_cols):
        first_copy(q).wait_recv()
    total = acc[row, :, col]
    for q in range(1, grid_cols):
        total = total + nw_recv[row, pl.ds(2 * q, 2)]
    sums = jnp.zeros((1, topics), F32)
    for b in range(2):
        at = pl.ds(pl.multiple_of((2 * col + b) * part, part), part)
        new = w_in[at] * total[b, :part] / total[b, part:part + 1]
        wfin[b] = new
        wb_ref[row, at] = new.astype(BF16)
        sums = sums + jnp.sum(new, axis=0, keepdims=True)
    ws_buf[row, 0] = jnp.broadcast_to(sums, (EXTRA, topics))
    for q in range(grid_cols):
        first_wb(row, q).start()
        first_ws(row, q).start()
    for b in range(2):
        @pl.when(2 * col + b == me)
        def _():
            wsl_ref[row] = wfin[b]

        @pl.when(2 * col + b != me)
        def _():
            first_owner(b).start()

    first_wb(1 - row, 0).wait_recv()
    first_ws(1 - row, 0).wait_recv()
    for q in range(1, grid_cols):
        first_wb(1 - row, q).start()
        first_ws(1 - row, q).start()
    for q in range(1, grid_cols):
        w0_forward(q).wait_recv()
    wbt0[1] = wb0[1].T
    ws0_ref[...] = to_lanes(ws0_buf[0] + ws0_buf[1])
    hs_first[...] = jnp.zeros_like(hs_first)
    for q in range(1, grid_cols):
        first_copy(q).wait_send()
    acc_zero(row)
    total = ws_buf[0, 0] + ws_buf[1, 0]
    for half in range(2):
        for q in range(1, grid_cols):
            first_wb(half, q).wait_recv()
            first_ws(half, q).wait_recv()
            total = total + ws_buf[half, q]
        wbt_ref[half] = wb_ref[half].T
    ws_ref[...] = to_lanes(total)

    def both_halves(slot, h):
        size = h.shape[1]
        hb = h.astype(BF16)
        q = ratio(cbuf[slot, :, pl.ds(0, size)], dot(wb_ref[row], hb))
        acc_add(row, dot_t(q, hb))
        nh = dot(wbt_ref[row], q)
        q = ratio(cbuf[slot, :, pl.ds(CHUNK, size)], dot(wb_ref[1 - row], hb))
        acc_add(1 - row, dot_t(q, hb))
        nh = nh + dot(wbt_ref[1 - row], q)
        return h * nh / ws_ref[:, :1]

    def chunk_step(j, carry):
        slot = lax.rem(j, 2)
        chunk_copy(j).wait_recv()
        par_chunk(j, slot, ARRIVE).start()
        chunk_copy(j).wait_send()

        @pl.when(j < arrivals // 2)
        def _():
            chunk_copy(j + AHEAD).start()

        @pl.when(jnp.logical_and(j >= arrivals // 2 + AHEAD - 2, j < arrivals - 2))
        def _():
            chunk_copy(j + 2).start()

        own_chunk(j, slot, ARRIVE).wait()

        @pl.when(j < arrivals - 1)
        def _():
            own_chunk(j + 1, 1 - slot, ARRIVE).start()

        at = pl.ds(pl.multiple_of(j * ARRIVE, ARRIVE), ARRIVE)
        h = h_ref[:, at]
        par_chunk(j, slot, ARRIVE).wait()
        other = cbuf[slot, :, pl.ds(CHUNK, ARRIVE)]
        q = ratio(other, dot(wb0[1], h.astype(BF16)))
        h = h * (nh_ref[:, at] + dot(wbt0[1], q)) / ws0_ref[:, :1]
        hs_first[...] += lane_sum(h)
        h = both_halves(slot, h)
        h_ref[:, at] = h
        hs_acc[...] += lane_sum(h)
        return carry

    lax.fori_loop(0, arrivals, chunk_step, 0)
    for copy in w0_copies():
        copy.wait_send()
    for q in range(1, grid_cols):
        w0_forward(q).wait_send()
    first_wb(row, 0).wait_send()
    first_ws(row, 0).wait_send()
    for half in range(2):
        for q in range(1, grid_cols):
            first_wb(half, q).wait_send()
            first_ws(half, q).wait_send()

        @pl.when(2 * col + half != me)
        def _():
            first_owner(half).wait_send()

        @pl.when(jnp.logical_not(wfin_here(half)))
        def _():
            remote(wfin.at[0], wsl_ref.at[half], wf_send.at[0], wf_got.at[half], partner).wait_recv()

    hs_row[...] = to_row(hs_first[...])
    send_nw(0)
    send_nw(1)
    c_start(0, 0, 0)
    relay(0)
    owner_update(0)

    def step(half, j, last):
        slot = lax.rem(j, 2)
        c_wait(slot)

        @pl.when(j < blocks - 1)
        def _():
            c_start(half, j + 1, 1 - slot)

        @pl.when(jnp.logical_and(j == blocks - 1, jnp.logical_not(last)))
        def _():
            c_start(1 - half, 0, 1 - slot)

        at = pl.ds(pl.multiple_of(j * BV, BV), BV)
        hb = h_ref[:, at].astype(BF16)
        q = ratio(cbuf[slot], dot(wb_ref[half], hb))
        acc_add(half, dot_t(q, hb))
        nh = dot(wbt_ref[half], q)
        if half == 0:
            nh_ref[:, at] = nh
        else:
            new = h_ref[:, at] * (nh_ref[:, at] + nh) / ws_ref[:, :1]
            h_ref[:, at] = new
            hs_acc[...] += lane_sum(new)

    def one_sweep(s, carry):
        last = s == sweeps - 1
        ws_half[...] = receive_w(0)
        sent_w(0)
        hs_row[...] = to_row(hs_acc[...])
        hs_acc[...] = jnp.zeros_like(hs_acc)
        sent_nw(0)
        acc_zero(0)

        def step_a(j, carry):
            @pl.when(j == RELAY_AT)
            def _():
                relay(1)

            @pl.when(j == UPDATE_AT)
            def _():
                owner_update(1)

            step(0, j, False)
            return carry

        lax.fori_loop(0, blocks, step_a, 0)
        send_nw(0)
        ws_ref[...] = to_lanes(ws_half[...] + receive_w(1))
        sent_w(1)
        sent_nw(1)
        acc_zero(1)

        def step_b(j, carry):
            @pl.when(j == RELAY_AT)
            def _():
                relay(0)

            @pl.when(j == UPDATE_AT)
            def _():
                owner_update(0)

            step(1, j, last)
            return carry

        lax.fori_loop(0, blocks, step_b, 0)
        send_nw(1)
        return carry

    lax.fori_loop(0, sweeps, one_sweep, 0)
    own_chunk(0, 0).start()
    par_chunk(0, 0).start()
    relay(1)
    owner_update(1)
    for half in range(2):
        @pl.when(wfin_here(half))
        def _():
            wfin[lax.rem(me, 2)] = wsl_ref[half]

        @pl.when(jnp.logical_not(wfin_here(half)))
        def _():
            wfin_copy(half).start()

    hs_row[...] = to_row(hs_acc[...])
    for half in range(2):
        sent_nw(half)
        acc_zero(half)
    ws_ref[...] = to_lanes(receive_w(0) + receive_w(1))

    def last_step(j, carry):
        slot = lax.rem(j, 2)
        own_chunk(j, slot).wait()
        par_chunk(j, slot).wait()

        @pl.when(j < chunks - 1)
        def _():
            own_chunk(j + 1, 1 - slot).start()
            par_chunk(j + 1, 1 - slot).start()

        @pl.when(j > 0)
        def _():
            h_remote(j - 1).start()
            h_local(j - 1).start()

        at = pl.ds(pl.multiple_of(j * CHUNK, CHUNK), CHUNK)
        h_ref[:, at] = both_halves(slot, h_ref[:, at])
        return carry

    lax.fori_loop(0, chunks, last_step, 0)
    for half in range(2):
        acc_sums(half)
    h_local(chunks - 1).start()
    tail = local(h_ref.at[:, pl.ds(width - CHUNK, CHUNK)], h_last, hhsem)
    tail.start()
    for q in range(1, grid_cols):
        fin_copy(q).start()
    for half in range(2):
        @pl.when(jnp.logical_not(wfin_here(half)))
        def _():
            wfin_copy(half).wait_send()

    for parity in range(2):
        @pl.when(2 * col + parity != me)
        def _():
            remote(wsl_ref.at[0], wfin.at[parity], wf_send.at[0], wf_got.at[parity], partner).wait_recv()

    for q in range(1, grid_cols):
        fin_copy(q).wait_recv()
    ours = acc[row, :, col]
    theirs = acc[1 - row, :, col]
    for q in range(1, grid_cols):
        ours = ours + nw_recv[row, pl.ds(2 * q, 2)]
        theirs = theirs + nw_recv[1 - row, pl.ds(2 * q, 2)]
    nw_recv[1 - row, pl.ds(0, 2)] = theirs
    fin_cross().start()
    fin_cross().wait_recv()
    total = ours + nw_recv[row, pl.ds(0, 2)]
    new = wfin[...] * total[:, :part] / total[:1, part:part + 1]
    for b in range(2):
        w_out[pl.ds(pl.multiple_of((2 * col + b) * part, part), part)] = new[b]
    for q in range(1, grid_cols):
        out_copy(q).start()
    for half in range(2):
        sent_w(half)
    for q in range(1, grid_cols):
        out_copy(q).wait()
        fin_copy(q).wait_send()
    fin_cross().wait_send()

    tail.wait()

    def drain(j, carry):
        h_remote(j).wait_recv()
        h_remote(j).wait_send()
        h_local(j).wait()
        return carry

    lax.fori_loop(0, chunks - 1, drain, 0)
    h_local(chunks - 1).wait()


PLACE = 2048


def place_kernel(h_pair, h_out, buf, in_sem, out_sem):
    row = lax.axis_index("row")
    width = h_pair.shape[2]
    jobs = []
    for other in range(2):
        half = 1 - row if other else row
        for start in range(0, width, PLACE):
            size = PLACE - CHUNK if other and start + PLACE == width else PLACE
            n = len(jobs)
            held = buf.at[n, :, pl.ds(0, size)]
            jobs.append((
                pltpu.make_async_copy(h_pair.at[half, :, pl.ds(start, size)], held, in_sem.at[n]),
                pltpu.make_async_copy(held, h_out.at[:, pl.ds(pl.multiple_of(half * width + start, PLACE), size)], out_sem.at[n]),
            ))
    for load, _ in jobs:
        load.start()
    for load, store in jobs:
        load.wait()
        store.start()
    for _, store in jobs:
        store.wait()


def cost(docs, columns, topics, dots):
    return pl.CostEstimate(flops=int(2 * docs * columns * topics * dots), bytes_accessed=2 * docs * columns, transcendentals=0)


def solution(mesh):
    rows, cols = mesh.shape["row"], mesh.shape["col"]

    def body(counts, w_own, h_blk):
        docs, width = counts.shape
        topics = w_own.shape[1]
        mine = width // rows
        sds = jax.ShapeDtypeStruct
        lanes = (topics, 128)
        part = docs // DEVICES
        vmem, hbm = pl.BlockSpec(memory_space=pltpu.VMEM), pl.BlockSpec(memory_space=pl.ANY)
        dma = pltpu.SemaphoreType.DMA
        V = pltpu.VMEM
        exchange = V((rows, DEVICES, part + EXTRA, topics), F32)
        partial = V((rows, 2, CHIPS, part + EXTRA, topics), F32)
        pieces = mine // CHUNK
        c_par, h_pair, h_last, w_out = pl.pallas_call(
            functools.partial(main_kernel, SWEEPS - 3, cols),
            in_specs=[hbm, vmem, hbm],
            out_specs=[hbm, hbm, hbm, vmem],
            out_shape=[sds((docs, mine), BF16), sds((rows, topics, mine), F32), sds((topics, CHUNK), F32),
                       sds((docs, topics), F32)],
            scratch_shapes=[
                V((topics, mine), F32), V((rows, docs, topics), BF16), V(lanes, F32), V(lanes, F32),
                V((rows, part, topics), F32), V((2, part, topics), F32),
                V((2, docs, BV), BF16), V((2, topics, BV), F32), V((topics, mine), F32), V((rows, topics, docs), BF16),
                V((2, docs, topics), BF16), V((2, topics, docs), BF16), V((2, EXTRA, topics), F32), V(lanes, F32),
                V(lanes, F32), partial, exchange, V((rows, DEVICES, EXTRA, topics), F32),
                V((EXTRA, topics), F32), V((EXTRA, topics), F32),
                dma((2,)), dma((2,)), dma((2,)), dma, dma((mine // ARRIVE,)), dma((mine // ARRIVE,)), dma((cols + 1,)), dma((cols + 1,)),
            ] + [dma((rows, DEVICES))] * 6 + [V((rows, CHIPS, part + EXTRA, topics), F32), dma((rows,)), dma((rows,))] + [dma((pieces,))] * 3 + [dma((2,))] * 2 + [dma((2 * cols,))] * 2,
            compiler_params=pltpu.CompilerParams(vmem_limit_bytes=VMEM, collective_id=0, has_side_effects=True),
            cost_estimate=cost(rows * docs, mine, topics, 18), name="main",
        )(counts, w_own, h_blk)
        other = lax.ppermute(h_last, "row", [(0, 1), (1, 0)])
        row = lax.axis_index("row")
        jobs = 2 * mine // PLACE
        h_out = pl.pallas_call(
            place_kernel,
            in_specs=[hbm], out_specs=hbm, out_shape=sds((topics, width), F32),
            scratch_shapes=[V((jobs, topics, PLACE), F32), dma((jobs,)), dma((jobs,))],
            compiler_params=pltpu.CompilerParams(vmem_limit_bytes=VMEM),
            cost_estimate=pl.CostEstimate(flops=10 ** 8, bytes_accessed=8 * topics * width, transcendentals=0), name="place",
        )(h_pair)
        h_out = lax.dynamic_update_slice(h_out, other, (0, (1 - row) * mine + mine - CHUNK))
        return w_out, h_out

    return jax.shard_map(
        body,
        mesh=mesh,
        in_specs=(P(("part", "row"), "col"), P(("part", "row"), None), P("part", "col")),
        out_specs=(P(("part", "row"), None), P("part", "col")),
        check_vma=False,
    )
```

```python
import functools

import jax
import jax.numpy as jnp
from jax import lax
from jax.experimental import pallas as pl
from jax.experimental.pallas import tpu as pltpu
from jax.sharding import PartitionSpec as P

SWEEPS = 6
F32 = jnp.float32
BF16 = jnp.bfloat16
BV = 1024
VMEM = 60 * 1024 * 1024


def dot(a, b):
    return jnp.dot(a, b, preferred_element_type=F32)


def dot_t(a, b):
    return lax.dot_general(a, b, (((1,), (1,)), ((), ())), preferred_element_type=F32)


def ratio(c, z):
    return (c.astype(F32) / z).astype(BF16)


def lane_sum(h):
    out = h[:, :128]
    for g in range(1, h.shape[1] // 128):
        out = out + h[:, g * 128:(g + 1) * 128]
    return out


DEVICES = 8
CHIPS = 4
EXTRA = 8
CHUNK = 512
ARRIVE = 256
AHEAD = 8
UPDATE_AT = 5
RELAY_AT = 0


def main_kernel(sweeps, grid_cols, counts, w_in, h_in,
                c_par, h_pair, h_last, w_out,
                h_ref, wb_ref, ws_ref, hs_acc, wsl_ref, wfin, cbuf, hbuf, nh_ref, wbt_ref, wb0, wbt0, ws0_buf, ws0_ref, hs_first, acc, nw_recv, ws_buf, ws_half, hs_row,
                csem, psem, hsem, hhsem, c_send, c_got, w0_send, w0_got,
                nw_send, nw_got, wb_send, wb_got, ws_send, ws_got,
                mate_recv, mate_send, mate_got, h_send, h_got, out_sem, wf_send, wf_got, fin_send, fin_got):
    row, col = lax.axis_index("row"), lax.axis_index("col")
    me = row * grid_cols + col
    docs, full = counts.shape
    topics, width = h_ref.shape
    blocks = width // BV
    chunks = width // CHUNK
    arrivals = width // ARRIVE
    part = docs // DEVICES
    partner = {"row": 1 - row, "col": col}
    mesh_id = pl.DeviceIdType.MESH

    def remote(src, dst, send, got, where):
        return pltpu.make_async_remote_copy(src, dst, send, got, device_id=where, device_id_type=mesh_id)

    def peer(p):
        other = lax.rem(me + p, DEVICES)
        return {"row": other // grid_cols, "col": lax.rem(other, grid_cols)}, other

    core, chip = lax.rem(col, 2), me // 2
    mate = {"row": row, "col": col + 1 - 2 * core}

    def mate_copy(half):
        return remote(acc.at[half, 1 - core], mate_recv.at[half], mate_send.at[half], mate_got.at[half], mate)

    def nw_copy(p, half):
        there = lax.rem(chip + p, CHIPS)
        d = 2 * there + core
        return remote(acc.at[half, core, there], nw_recv.at[half, p], nw_send.at[half, p], nw_got.at[half, p],
                      {"row": d // grid_cols, "col": lax.rem(d, grid_cols)})

    def wb_copy(p, half):
        mine = wb_ref.at[half, pl.ds(pl.multiple_of(me * part, part), part)]
        return remote(mine, mine, wb_send.at[half, p], wb_got.at[half, p], peer(p)[0])

    def ws_copy(p, half):
        return remote(ws_buf.at[half, 0], ws_buf.at[half, p], ws_send.at[half, p], ws_got.at[half, p], peer(p)[0])

    def row_peer(q):
        there = lax.rem(col + q, grid_cols)
        return {"row": row, "col": there}, there

    def first_copy(q):
        where, there = row_peer(q)
        return remote(acc.at[row, :, there], nw_recv.at[row, pl.ds(2 * q, 2)], fin_send.at[q], fin_got.at[q], where)

    def first_wb(half, q):
        where = row_peer(q)[0] if q else partner
        mine = wb_ref.at[half, pl.ds(pl.multiple_of(col * 2 * part, 2 * part), 2 * part)]
        return remote(mine, mine, wb_send.at[half, q], wb_got.at[half, q], where)

    def first_ws(half, q):
        where = row_peer(q)[0] if q else partner
        return remote(ws_buf.at[half, 0], ws_buf.at[half, q], ws_send.at[half, q], ws_got.at[half, q], where)

    def first_owner(b):
        d = 2 * col + b
        return remote(wfin.at[b], wsl_ref.at[row], wf_send.at[b], wf_got.at[row],
                      {"row": d // grid_cols, "col": lax.rem(d, grid_cols)})

    def chunk_copy(j):
        theirs = pl.ds(pl.multiple_of((1 - row) * width + j * ARRIVE, ARRIVE), ARRIVE)
        here = pl.ds(pl.multiple_of(j * ARRIVE, ARRIVE), ARRIVE)
        return remote(counts.at[:, theirs], c_par.at[:, here], c_send.at[j], c_got.at[j], partner)

    def w0_copies():
        at = pl.ds(pl.multiple_of(col * 2 * part, 2 * part), 2 * part)
        return [
            remote(wb0.at[0, at], wb0.at[1, at], w0_send.at[0], w0_got.at[0], partner),
            remote(ws0_buf.at[0], ws0_buf.at[1], w0_send.at[grid_cols], w0_got.at[grid_cols], partner),
        ]

    def w0_forward(q):
        at = pl.ds(pl.multiple_of(col * 2 * part, 2 * part), 2 * part)
        return remote(wb0.at[1, at], wb0.at[1, at], w0_send.at[q], w0_got.at[q], row_peer(q)[0])

    def local(src, dst, sem):
        return pltpu.make_async_copy(src, dst, sem)

    def c_start(half, j, slot):
        @pl.when(row == half)
        def _():
            local(counts.at[:, pl.ds(pl.multiple_of(row * width + j * BV, BV), BV)], cbuf.at[slot], csem.at[slot]).start()

        @pl.when(row != half)
        def _():
            local(c_par.at[:, pl.ds(pl.multiple_of(j * BV, BV), BV)], cbuf.at[slot], csem.at[slot]).start()

    def c_wait(slot):
        local(counts.at[:, pl.ds(0, BV)], cbuf.at[slot], csem.at[slot]).wait()

    def first_c(i, slot):
        block = lax.rem(row * blocks + i, 2 * blocks)
        return local(counts.at[:, pl.ds(pl.multiple_of(block * BV, BV), BV)], cbuf.at[slot], csem.at[slot])

    def first_h(j, slot):
        at = pl.ds(pl.multiple_of((1 - row) * width + j * BV, BV), BV)
        return local(h_in.at[:, at], hbuf.at[slot], hsem.at[slot])

    def own_chunk(j, slot, size=CHUNK):
        at = pl.ds(pl.multiple_of(row * width + j * size, size), size)
        return local(counts.at[:, at], cbuf.at[slot, :, pl.ds(0, size)], csem.at[slot])

    def par_chunk(j, slot, size=CHUNK):
        at = pl.ds(pl.multiple_of(j * size, size), size)
        return local(c_par.at[:, at], cbuf.at[slot, :, pl.ds(CHUNK, size)], psem.at[slot])

    def acc_add(half, res):
        for b in range(DEVICES):
            acc[half, b % 2, b // 2, pl.ds(0, part)] += res[b * part:(b + 1) * part]

    def acc_sums(half):
        for b in range(DEVICES):
            acc[half, b % 2, b // 2, pl.ds(part, EXTRA)] = hs_row[...]

    def acc_zero(half):
        acc[half] = jnp.zeros(acc.shape[1:], F32)

    def send_nw(half):
        acc_sums(half)
        mate_copy(half).start()

    def relay(half):
        mate_copy(half).wait_recv()
        acc[half, core] += mate_recv[half]
        for p in range(1, CHIPS):
            nw_copy(p, half).start()

    def publish(half, total):
        new = wsl_ref[half] * total[:part] / total[part:part + 1]
        wsl_ref[half] = new
        wb_ref[half, pl.ds(pl.multiple_of(me * part, part), part)] = new.astype(BF16)
        ws_buf[half, 0] = jnp.broadcast_to(jnp.sum(new, axis=0, keepdims=True), (EXTRA, topics))
        for p in range(1, DEVICES):
            wb_copy(p, half).start()
            ws_copy(p, half).start()

    def sent_w(half):
        for p in range(1, DEVICES):
            wb_copy(p, half).wait_send()
            ws_copy(p, half).wait_send()

    def sent_nw(half):
        mate_copy(half).wait_send()
        for p in range(1, CHIPS):
            nw_copy(p, half).wait_send()

    def owner_update(half):
        for p in range(1, CHIPS):
            nw_copy(p, half).wait_recv()
        total = acc[half, core, chip]
        for p in range(1, CHIPS):
            total = total + nw_recv[half, p]
        publish(half, total)

    def receive_w(half):
        for p in range(1, DEVICES):
            wb_copy(p, half).wait_recv()
            ws_copy(p, half).wait_recv()
        wbt_ref[half] = wb_ref[half].T
        total = ws_buf[half, 0]
        for p in range(1, DEVICES):
            total = total + ws_buf[half, p]
        return total

    def wfin_copy(half):
        return remote(wsl_ref.at[half], wfin.at[lax.rem(me, 2)], wf_send.at[half], wf_got.at[lax.rem(me, 2)],
                      {"row": jnp.int32(half), "col": me // 2})

    def wfin_here(half):
        return jnp.logical_and(row == half, col == me // 2)

    def fin_copy(q):
        there = lax.rem(col + q, grid_cols)
        return remote(acc.at[:, :, there], nw_recv.at[:, pl.ds(2 * q, 2)], fin_send.at[q], fin_got.at[q],
                      {"row": row, "col": there})

    def fin_cross():
        pair = nw_recv.at[1 - row, pl.ds(0, 2)]
        return remote(pair, pair, fin_send.at[0], fin_got.at[0], partner)

    def out_copy(q):
        mine = w_out.at[pl.ds(pl.multiple_of(col * 2 * part, 2 * part), 2 * part)]
        return remote(mine, mine, fin_send.at[grid_cols + q], fin_got.at[grid_cols + q],
                      {"row": row, "col": lax.rem(col + q, grid_cols)})

    def h_remote(j):
        at = pl.ds(pl.multiple_of(j * CHUNK, CHUNK), CHUNK)
        return remote(h_ref.at[:, at], h_pair.at[row, :, at], h_send.at[j], h_got.at[j], partner)

    def h_local(j):
        at = pl.ds(pl.multiple_of(j * CHUNK, CHUNK), CHUNK)
        return local(h_ref.at[:, at], h_pair.at[row, :, at], out_sem.at[j])

    def to_row(lanes):
        return jnp.broadcast_to(jnp.sum(lanes.T, axis=0, keepdims=True), (EXTRA, topics))

    def to_lanes(sums):
        return jnp.broadcast_to(sums[:1], (128, topics)).T

    barrier = pltpu.get_barrier_semaphore()
    for p in range(1, DEVICES):
        pl.semaphore_signal(barrier, inc=1, device_id=peer(p)[0], device_id_type=mesh_id)

    own_h = local(h_in.at[:, pl.ds(pl.multiple_of(row * width, width), width)], h_ref, hhsem)
    own_h.start()
    first_c(0, 0).start()
    wb0[0] = w_in[...].astype(BF16)
    ws0_buf[0] = jnp.broadcast_to(jnp.sum(w_in[...], axis=0, keepdims=True), (EXTRA, topics))
    pl.semaphore_wait(barrier, DEVICES - 1)
    for copy in w0_copies():
        copy.start()
    for j in range(AHEAD):
        chunk_copy(j).start()
    wbt0[0] = wb0[0].T
    acc_zero(0)
    acc_zero(1)
    hs_first[...] = jnp.zeros_like(hs_first)
    hs_acc[...] = jnp.zeros_like(hs_acc)
    own_h.wait()

    def first_own(j, carry):
        slot = lax.rem(j, 2)
        first_c(j, slot).wait()
        first_c(j + 1, 1 - slot).start()

        @pl.when(j == blocks - 1)
        def _():
            first_h(0, 0).start()

        at = pl.ds(pl.multiple_of(j * BV, BV), BV)
        h = h_ref[:, at]
        hb = h.astype(BF16)
        q = ratio(cbuf[slot], dot(wb0[0], hb))
        acc_add(row, dot_t(q, hb))
        nh_ref[:, at] = dot(wbt0[0], q)
        hs_first[...] += lane_sum(h)
        return carry

    lax.fori_loop(0, blocks, first_own, 0)

    def first_other(j, carry):
        slot = lax.rem(j, 2)
        first_c(blocks + j, slot).wait()
        first_h(j, slot).wait()

        @pl.when(j < blocks - 1)
        def _():
            first_c(blocks + j + 1, 1 - slot).start()
            first_h(j + 1, 1 - slot).start()

        h = hbuf[slot]
        hb = h.astype(BF16)
        q = ratio(cbuf[slot], dot(wb0[0], hb))
        acc_add(row, dot_t(q, hb))
        hs_first[...] += lane_sum(h)
        return carry

    lax.fori_loop(0, blocks, first_other, 0)

    hs_row[...] = to_row(hs_first[...])
    acc_sums(row)
    for q in range(1, grid_cols):
        first_copy(q).start()
    own_chunk(0, 0, ARRIVE).start()
    for copy in w0_copies():
        copy.wait_recv()
    for q in range(1, grid_cols):
        w0_forward(q).start()
    for q in range(1, grid_cols):
        first_copy(q).wait_recv()
    total = acc[row, :, col]
    for q in range(1, grid_cols):
        total = total + nw_recv[row, pl.ds(2 * q, 2)]
    sums = jnp.zeros((1, topics), F32)
    for b in range(2):
        at = pl.ds(pl.multiple_of((2 * col + b) * part, part), part)
        new = w_in[at] * total[b, :part] / total[b, part:part + 1]
        wfin[b] = new
        wb_ref[row, at] = new.astype(BF16)
        sums = sums + jnp.sum(new, axis=0, keepdims=True)
    ws_buf[row, 0] = jnp.broadcast_to(sums, (EXTRA, topics))
    for q in range(grid_cols):
        first_wb(row, q).start()
        first_ws(row, q).start()
    for b in range(2):
        @pl.when(2 * col + b == me)
        def _():
            wsl_ref[row] = wfin[b]

        @pl.when(2 * col + b != me)
        def _():
            first_owner(b).start()

    first_wb(1 - row, 0).wait_recv()
    first_ws(1 - row, 0).wait_recv()
    for q in range(1, grid_cols):
        first_wb(1 - row, q).start()
        first_ws(1 - row, q).start()
    for q in range(1, grid_cols):
        w0_forward(q).wait_recv()
    wbt0[1] = wb0[1].T
    ws0_ref[...] = to_lanes(ws0_buf[0] + ws0_buf[1])
    hs_first[...] = jnp.zeros_like(hs_first)
    for q in range(1, grid_cols):
        first_copy(q).wait_send()
    acc_zero(row)
    total = ws_buf[0, 0] + ws_buf[1, 0]
    for half in range(2):
        for q in range(1, grid_cols):
            first_wb(half, q).wait_recv()
            first_ws(half, q).wait_recv()
            total = total + ws_buf[half, q]
        wbt_ref[half] = wb_ref[half].T
    ws_ref[...] = to_lanes(total)

    def both_halves(slot, h):
        size = h.shape[1]
        hb = h.astype(BF16)
        q = ratio(cbuf[slot, :, pl.ds(0, size)], dot(wb_ref[row], hb))
        acc_add(row, dot_t(q, hb))
        nh = dot(wbt_ref[row], q)
        q = ratio(cbuf[slot, :, pl.ds(CHUNK, size)], dot(wb_ref[1 - row], hb))
        acc_add(1 - row, dot_t(q, hb))
        nh = nh + dot(wbt_ref[1 - row], q)
        return h * nh / ws_ref[:, :1]

    def chunk_step(j, carry):
        slot = lax.rem(j, 2)
        chunk_copy(j).wait_recv()
        par_chunk(j, slot, ARRIVE).start()
        chunk_copy(j).wait_send()

        @pl.when(j < arrivals // 2)
        def _():
            chunk_copy(j + AHEAD).start()

        @pl.when(jnp.logical_and(j >= arrivals // 2 + AHEAD - 2, j < arrivals - 2))
        def _():
            chunk_copy(j + 2).start()

        own_chunk(j, slot, ARRIVE).wait()

        @pl.when(j < arrivals - 1)
        def _():
            own_chunk(j + 1, 1 - slot, ARRIVE).start()

        at = pl.ds(pl.multiple_of(j * ARRIVE, ARRIVE), ARRIVE)
        h = h_ref[:, at]
        par_chunk(j, slot, ARRIVE).wait()
        other = cbuf[slot, :, pl.ds(CHUNK, ARRIVE)]
        q = ratio(other, dot(wb0[1], h.astype(BF16)))
        h = h * (nh_ref[:, at] + dot(wbt0[1], q)) / ws0_ref[:, :1]
        hs_first[...] += lane_sum(h)
        h = both_halves(slot, h)
        h_ref[:, at] = h
        hs_acc[...] += lane_sum(h)
        return carry

    lax.fori_loop(0, arrivals, chunk_step, 0)
    for copy in w0_copies():
        copy.wait_send()
    for q in range(1, grid_cols):
        w0_forward(q).wait_send()
    first_wb(row, 0).wait_send()
    first_ws(row, 0).wait_send()
    for half in range(2):
        for q in range(1, grid_cols):
            first_wb(half, q).wait_send()
            first_ws(half, q).wait_send()

        @pl.when(2 * col + half != me)
        def _():
            first_owner(half).wait_send()

        @pl.when(jnp.logical_not(wfin_here(half)))
        def _():
            remote(wfin.at[0], wsl_ref.at[half], wf_send.at[0], wf_got.at[half], partner).wait_recv()

    hs_row[...] = to_row(hs_first[...])
    send_nw(0)
    send_nw(1)
    c_start(0, 0, 0)
    relay(0)
    owner_update(0)

    def step(half, j, last):
        slot = lax.rem(j, 2)
        c_wait(slot)

        @pl.when(j < blocks - 1)
        def _():
            c_start(half, j + 1, 1 - slot)

        @pl.when(jnp.logical_and(j == blocks - 1, jnp.logical_not(last)))
        def _():
            c_start(1 - half, 0, 1 - slot)

        at = pl.ds(pl.multiple_of(j * BV, BV), BV)
        hb = h_ref[:, at].astype(BF16)
        q = ratio(cbuf[slot], dot(wb_ref[half], hb))
        acc_add(half, dot_t(q, hb))
        nh = dot(wbt_ref[half], q)
        if half == 0:
            nh_ref[:, at] = nh
        else:
            new = h_ref[:, at] * (nh_ref[:, at] + nh) / ws_ref[:, :1]
            h_ref[:, at] = new
            hs_acc[...] += lane_sum(new)

    def one_sweep(s, carry):
        last = s == sweeps - 1
        ws_half[...] = receive_w(0)
        sent_w(0)
        hs_row[...] = to_row(hs_acc[...])
        hs_acc[...] = jnp.zeros_like(hs_acc)
        sent_nw(0)
        acc_zero(0)

        def step_a(j, carry):
            @pl.when(j == RELAY_AT)
            def _():
                relay(1)

            @pl.when(j == UPDATE_AT)
            def _():
                owner_update(1)

            step(0, j, False)
            return carry

        lax.fori_loop(0, blocks, step_a, 0)
        send_nw(0)
        ws_ref[...] = to_lanes(ws_half[...] + receive_w(1))
        sent_w(1)
        sent_nw(1)
        acc_zero(1)

        def step_b(j, carry):
            @pl.when(j == RELAY_AT)
            def _():
                relay(0)

            @pl.when(j == UPDATE_AT)
            def _():
                owner_update(0)

            step(1, j, last)
            return carry

        lax.fori_loop(0, blocks, step_b, 0)
        send_nw(1)
        return carry

    lax.fori_loop(0, sweeps, one_sweep, 0)
    own_chunk(0, 0).start()
    par_chunk(0, 0).start()
    relay(1)
    owner_update(1)
    for half in range(2):
        @pl.when(wfin_here(half))
        def _():
            wfin[lax.rem(me, 2)] = wsl_ref[half]

        @pl.when(jnp.logical_not(wfin_here(half)))
        def _():
            wfin_copy(half).start()

    hs_row[...] = to_row(hs_acc[...])
    for half in range(2):
        sent_nw(half)
        acc_zero(half)
    ws_ref[...] = to_lanes(receive_w(0) + receive_w(1))

    def last_step(j, carry):
        slot = lax.rem(j, 2)
        own_chunk(j, slot).wait()
        par_chunk(j, slot).wait()

        @pl.when(j < chunks - 1)
        def _():
            own_chunk(j + 1, 1 - slot).start()
            par_chunk(j + 1, 1 - slot).start()

        @pl.when(j > 0)
        def _():
            h_remote(j - 1).start()
            h_local(j - 1).start()

        at = pl.ds(pl.multiple_of(j * CHUNK, CHUNK), CHUNK)
        h_ref[:, at] = both_halves(slot, h_ref[:, at])
        return carry

    lax.fori_loop(0, chunks, last_step, 0)
    for half in range(2):
        acc_sums(half)
    h_local(chunks - 1).start()
    tail = local(h_ref.at[:, pl.ds(width - CHUNK, CHUNK)], h_last, hhsem)
    tail.start()
    for q in range(1, grid_cols):
        fin_copy(q).start()
    for half in range(2):
        @pl.when(jnp.logical_not(wfin_here(half)))
        def _():
            wfin_copy(half).wait_send()

    for parity in range(2):
        @pl.when(2 * col + parity != me)
        def _():
            remote(wsl_ref.at[0], wfin.at[parity], wf_send.at[0], wf_got.at[parity], partner).wait_recv()

    for q in range(1, grid_cols):
        fin_copy(q).wait_recv()
    ours = acc[row, :, col]
    theirs = acc[1 - row, :, col]
    for q in range(1, grid_cols):
        ours = ours + nw_recv[row, pl.ds(2 * q, 2)]
        theirs = theirs + nw_recv[1 - row, pl.ds(2 * q, 2)]
    nw_recv[1 - row, pl.ds(0, 2)] = theirs
    fin_cross().start()
    fin_cross().wait_recv()
    total = ours + nw_recv[row, pl.ds(0, 2)]
    new = wfin[...] * total[:, :part] / total[:1, part:part + 1]
    for b in range(2):
        w_out[pl.ds(pl.multiple_of((2 * col + b) * part, part), part)] = new[b]
    for q in range(1, grid_cols):
        out_copy(q).start()
    for half in range(2):
        sent_w(half)
    for q in range(1, grid_cols):
        out_copy(q).wait()
        fin_copy(q).wait_send()
    fin_cross().wait_send()

    tail.wait()

    def drain(j, carry):
        h_remote(j).wait_recv()
        h_remote(j).wait_send()
        h_local(j).wait()
        return carry

    lax.fori_loop(0, chunks - 1, drain, 0)
    h_local(chunks - 1).wait()


PLACE = 2048


def place_kernel(h_pair, w_in, h_out, w_out, buf, w_buf, in_sem, out_sem):
    row = lax.axis_index("row")
    width = h_pair.shape[2]
    jobs = []
    for other in range(2):
        half = 1 - row if other else row
        for start in range(0, width, PLACE):
            size = PLACE - CHUNK if other and start + PLACE == width else PLACE
            n = len(jobs)
            held = buf.at[n, :, pl.ds(0, size)]
            jobs.append((
                pltpu.make_async_copy(h_pair.at[half, :, pl.ds(start, size)], held, in_sem.at[n]),
                pltpu.make_async_copy(held, h_out.at[:, pl.ds(pl.multiple_of(half * width + start, PLACE), size)], out_sem.at[n]),
            ))
    n = len(jobs)
    jobs.append((pltpu.make_async_copy(w_in, w_buf, in_sem.at[n]), pltpu.make_async_copy(w_buf, w_out, out_sem.at[n])))
    for load, _ in jobs:
        load.start()
    for load, store in jobs:
        load.wait()
        store.start()
    for _, store in jobs:
        store.wait()


def cost(docs, columns, topics, dots):
    return pl.CostEstimate(flops=int(2 * docs * columns * topics * dots), bytes_accessed=2 * docs * columns, transcendentals=0)


def solution(mesh):
    rows, cols = mesh.shape["row"], mesh.shape["col"]

    def body(counts, w_own, h_blk):
        docs, width = counts.shape
        topics = w_own.shape[1]
        mine = width // rows
        sds = jax.ShapeDtypeStruct
        lanes = (topics, 128)
        part = docs // DEVICES
        vmem, hbm = pl.BlockSpec(memory_space=pltpu.VMEM), pl.BlockSpec(memory_space=pl.ANY)
        dma = pltpu.SemaphoreType.DMA
        V = pltpu.VMEM
        exchange = V((rows, DEVICES, part + EXTRA, topics), F32)
        partial = V((rows, 2, CHIPS, part + EXTRA, topics), F32)
        pieces = mine // CHUNK
        c_par, h_pair, h_last, w_out = pl.pallas_call(
            functools.partial(main_kernel, SWEEPS - 3, cols),
            in_specs=[hbm, vmem, hbm],
            out_specs=[hbm, hbm, hbm, vmem],
            out_shape=[sds((docs, mine), BF16), sds((rows, topics, mine), F32), sds((topics, CHUNK), F32),
                       sds((docs, topics), F32)],
            scratch_shapes=[
                V((topics, mine), F32), V((rows, docs, topics), BF16), V(lanes, F32), V(lanes, F32),
                V((rows, part, topics), F32), V((2, part, topics), F32),
                V((2, docs, BV), BF16), V((2, topics, BV), F32), V((topics, mine), F32), V((rows, topics, docs), BF16),
                V((2, docs, topics), BF16), V((2, topics, docs), BF16), V((2, EXTRA, topics), F32), V(lanes, F32),
                V(lanes, F32), partial, exchange, V((rows, DEVICES, EXTRA, topics), F32),
                V((EXTRA, topics), F32), V((EXTRA, topics), F32),
                dma((2,)), dma((2,)), dma((2,)), dma, dma((mine // ARRIVE,)), dma((mine // ARRIVE,)), dma((cols + 1,)), dma((cols + 1,)),
            ] + [dma((rows, DEVICES))] * 6 + [V((rows, CHIPS, part + EXTRA, topics), F32), dma((rows,)), dma((rows,))] + [dma((pieces,))] * 3 + [dma((2,))] * 2 + [dma((2 * cols,))] * 2,
            compiler_params=pltpu.CompilerParams(vmem_limit_bytes=VMEM, collective_id=0, has_side_effects=True),
            cost_estimate=cost(rows * docs, mine, topics, 18), name="main",
        )(counts, w_own, h_blk)
        other = lax.ppermute(h_last, "row", [(0, 1), (1, 0)])
        row = lax.axis_index("row")
        jobs = 2 * mine // PLACE
        h_out, w_out = pl.pallas_call(
            place_kernel,
            in_specs=[hbm, hbm], out_specs=[hbm, hbm],
            out_shape=[sds((topics, width), F32), sds((docs, topics), F32)],
            scratch_shapes=[V((jobs, topics, PLACE), F32), V((docs, topics), F32), dma((jobs + 1,)), dma((jobs + 1,))],
            compiler_params=pltpu.CompilerParams(vmem_limit_bytes=VMEM),
            cost_estimate=pl.CostEstimate(flops=10 ** 8, bytes_accessed=8 * topics * width, transcendentals=0), name="place",
        )(h_pair, w_out)
        h_out = lax.dynamic_update_slice(h_out, other, (0, (1 - row) * mine + mine - CHUNK))
        return w_out, h_out

    return jax.shard_map(
        body,
        mesh=mesh,
        in_specs=(P(("part", "row"), "col"), P(("part", "row"), None), P("part", "col")),
        out_specs=(P(("part", "row"), None), P("part", "col")),
        check_vma=False,
    )
```
